32 devices in a mesh: grp: 2 (over y), seq: 8 (over z, x), head: 2 (over core).
Axes of the slice: x: 2, y: 2, z: 4, core: 2. Of those that a mesh axis runs over, the one named last changes fastest.
Arguments:
- query_rows: bfloat16 [16, 32, 128], P('grp', 'head'), parts along dimension 0, may hold values from -100 to 100
- cache_keys: bfloat16 [512, 8, 128, 128], P(('grp', 'seq'), 'head'), parts along dimension 0, may hold values from -5 to 5
- cache_values: bfloat16 [512, 8, 128, 128], P(('grp', 'seq'), 'head'), parts along dimension 0, may hold values from -6 to 6
- page_table: int32 [512], P('grp'), parts along dimension 0, may hold values from 0 to 255, as said below
- seq_lengths: int32 [16], P('grp'), parts along dimension 0, may hold values from 128 to 4096, as said below
Outputs:
- attended: bfloat16 [16, 32, 128], P('grp', 'head'), parts along dimension 0
The draws below stay inside these ranges and needn't reach their ends.
There are 2 independent parts, one for each index of `grp`. The reference program is written for one: setup_inputs(seed, part) draws one part's arguments, and reference() takes and returns one part's arrays. A program takes and returns all parts, laid end to end along the dimension named above; each array names one. Nothing has to cross between parts.
Inputs may be any that keep to these rules, and one draw needn't show every extreme that they name: `page_table`: entry b * 32 + j is the pool slot of page j of sequence b; slot s lies on index s // 32 of seq; every slot appears once. `seq_lengths`: some sequence has exactly 4096 tokens.
All inputs are finite; a program needn't handle non-finite values.
Results may differ from the reference program's by a relative error of at most 0.0029.
Values may be sent and summed in bfloat16 or wider, within the bound.
A program may use at most 64 MiB of HBM per device.

```python
import math
import jax
import jax.numpy as jnp
from jax import lax

H = 32
KVH = 8
HD = 128
PAGE = 128
BATCH = 8
POOL = 256
MAXP = 32


def slot_layout(key):
    return jax.random.permutation(jax.random.fold_in(key, 7), POOL).astype(jnp.int32)


def draw_page_table(key, part):
    return slot_layout(key)


def draw_seq_lengths(key, part):
    drawn = jax.random.randint(jax.random.fold_in(key, 5), (BATCH,), PAGE, MAXP * PAGE + 1)
    return drawn.at[0].set(MAXP * PAGE).astype(jnp.int32)


def draw_query_rows(key, part):
    values = jnp.clip(3.0 * jax.random.normal(jax.random.fold_in(key, 13), (BATCH, H, HD), jnp.float32), -15.0, 15.0)
    return values.astype(jnp.bfloat16)


def draw_cache_keys(key, part):
    values = jnp.clip(jax.random.normal(jax.random.fold_in(key, 17), (POOL, KVH, PAGE, HD), jnp.float32), -5.0, 5.0)
    return values.astype(jnp.bfloat16)


def shard_levels(key, shape, pieces, low, high):
    factor_of, own = 1.0, jax.random.fold_in(key, 6)
    for axis_at, shards_of in pieces:
        draws = jnp.exp(jax.random.uniform(jax.random.fold_in(own, axis_at), (shards_of,), jnp.float32, low / len(pieces), high / len(pieces)))
        factor_of = factor_of * jnp.repeat(draws, shape[axis_at] // shards_of).reshape([-1 if axis == axis_at else 1 for axis in range(len(shape))])
    return factor_of


def scatter_about(stream_key, shape, scale, limit, shards=(), kind=jnp.bfloat16):
    result = scale * jax.random.normal(stream_key, shape, jnp.float32)
    if shards:
        result = result * shard_levels(stream_key, shape, shards, -0.22, 0.18)
    return jnp.clip(result, -limit, limit).astype(kind)


def setup_inputs(seed: int = 0, part: int = 0) -> dict:
    key_of = jax.random.split(jax.random.key(seed), 6)
    own_keys = jax.random.split(jax.random.fold_in(key_of[5], part), 6)
    return {
        "query_rows": draw_query_rows(jax.random.fold_in(jax.random.fold_in(key_of[5], part), 71), part),
        "cache_keys": draw_cache_keys(jax.random.fold_in(jax.random.fold_in(key_of[5], part), 71), part),
        "cache_values": scatter_about(own_keys[2], (POOL, KVH, PAGE, HD), 1.0, 6.0, ((0, 8), (1, 2))),
        "page_table": draw_page_table(jax.random.fold_in(jax.random.fold_in(key_of[5], part), 71), part),
        "seq_lengths": draw_seq_lengths(jax.random.fold_in(jax.random.fold_in(key_of[5], part), 71), part),
    }


def reference(query_rows, cache_keys, cache_values, page_table, seq_lengths):
    group_size = H // KVH
    score_scale = 1.0 / math.sqrt(HD)
    positions = jnp.arange(MAXP * PAGE, dtype=jnp.int32)

    def per_sequence(seq_index):
        slots = lax.dynamic_slice_in_dim(page_table, (seq_index * MAXP).astype(jnp.int32), MAXP)
        keys_here = jnp.take(cache_keys, slots, axis=0).astype(jnp.float32)
        keys_here = keys_here.transpose(1, 0, 2, 3).reshape(KVH, MAXP * PAGE, HD)
        values_here = jnp.take(cache_values, slots, axis=0).astype(jnp.float32)
        values_here = values_here.transpose(1, 0, 2, 3).reshape(KVH, MAXP * PAGE, HD)
        queries = query_rows[seq_index].astype(jnp.float32).reshape(KVH, group_size, HD)
        scores = jnp.einsum('gqd,gpd->gqp', queries, keys_here, precision=lax.Precision.HIGHEST) * score_scale
        is_live = positions < seq_lengths[seq_index]
        row_top = lax.optimization_barrier(jnp.max(jnp.where(is_live, scores, -jnp.inf), axis=-1, keepdims=True))
        weights = jnp.where(is_live, jnp.exp(scores - row_top), 0.0)
        totals = lax.optimization_barrier(jnp.sum(weights, axis=-1))
        rounded = lax.optimization_barrier(weights.astype(jnp.bfloat16)).astype(jnp.float32)
        numerators = jnp.einsum('gqp,gpd->gqd', rounded, values_here, precision=lax.Precision.HIGHEST)
        return (numerators / totals[..., None]).reshape(H, HD).astype(jnp.bfloat16)
    return lax.map(per_sequence, jnp.arange(BATCH, dtype=jnp.int32))
```

```python
import functools
import math

import jax
import jax.numpy as jnp
from jax import lax
from jax.experimental import pallas as pl
from jax.experimental.pallas import tpu as pltpu
from jax.sharding import PartitionSpec as P

MESH = pl.DeviceIdType.MESH
VERY_LOW = -1e30
FLOOR = -1e29
KEY_PIECES = 8
VALUE_PIECES = ((1, 1, 1, 1), (2, 2, 2, 1, 1))
VALUE_LEAD = 0
PAUSE = 100


def attend(
    n,
    table_width,
    owners,
    pick_acc,
    score_acc,
    value_acc,
    q_hbm,
    k_hbm,
    v_hbm,
    pt_hbm,
    len_hbm,
    out_ref,
    q_raw,
    pt_vmem,
    len_smem,
    k_vmem,
    v_vmem,
    slot_seq,
    slot_live,
    picked,
    choose,
    soft,
    spread,
    bias,
    crest,
    row_vmem,
    row_smem,
    stat_out,
    stat_in,
    num_out,
    num_in,
    small_sem,
    k_sem,
    v_sem,
    stat_send,
    stat_recv,
    num_send,
    num_recv,
    fin_send,
    fin_recv,
):
    me = lax.axis_index("seq")
    batch, heads, head_dim = q_raw.shape
    slots, kv_heads, page, _ = k_vmem.shape
    pairs = kv_heads // 2
    half = heads // kv_heads
    rows = 2 * half
    pool = pt_vmem.shape[0]
    parts = len(owners)
    share = batch // parts
    f32, bf16 = jnp.float32, jnp.bfloat16
    factor = math.log2(math.e) / math.sqrt(head_dim)

    small = (
        pltpu.make_async_copy(pt_hbm, pt_vmem, small_sem.at[0]),
        pltpu.make_async_copy(len_hbm, len_smem, small_sem.at[1]),
        pltpu.make_async_copy(q_hbm, q_raw, small_sem.at[2]),
    )
    for copy in small:
        copy.start()
    pl.delay(PAUSE)
    span = slots // KEY_PIECES
    k_copies = [
        pltpu.make_async_copy(
            k_hbm.at[pl.ds(i * span, span)], k_vmem.at[pl.ds(i * span, span)], k_sem.at[i]
        )
        for i in range(KEY_PIECES)
    ]
    v_copies = []
    for j in range(pairs):
        cuts = VALUE_PIECES[min(j, 1)]
        unit, at = slots // sum(cuts), 0
        for size in cuts:
            pages = pl.ds(at, size * unit)
            v_copies.append(
                (
                    j,
                    at,
                    size * unit,
                    pltpu.make_async_copy(
                        v_hbm.at[pages, pl.ds(2 * j, 2)],
                        v_vmem.at[pages, pl.ds(2 * j, 2)],
                        v_sem.at[len(v_copies)],
                    ),
                )
            )
            at += size * unit
    for copy in k_copies:
        copy.start()
    unstarted = [copy for _, _, _, copy in v_copies]

    mine = functools.reduce(lambda a, b: a | b, [me == o for o in owners])
    rank = sum(jnp.where(me == o, i, 0) for i, o in enumerate(owners))
    barrier = pltpu.get_barrier_semaphore()

    @pl.when(mine)
    def _():
        for step in range(1, n):
            pl.semaphore_signal(
                barrier, inc=1, device_id={"seq": lax.rem(me + step, n)}, device_id_type=MESH
            )

    def stat_copy(i, slot):
        return pltpu.make_async_remote_copy(
            src_ref=stat_out.at[i],
            dst_ref=stat_in.at[slot],
            send_sem=stat_send.at[i],
            recv_sem=stat_recv.at[slot],
            device_id={"seq": owners[i]},
            device_id_type=MESH,
        )

    def num_copy(j, i, slot):
        return pltpu.make_async_remote_copy(
            src_ref=num_out.at[j, i],
            dst_ref=num_in.at[j, slot],
            send_sem=num_send.at[j, i],
            recv_sem=num_recv.at[j, slot],
            device_id={"seq": owners[i]},
            device_id_type=MESH,
        )

    def fin_copy(dest, i):
        block = out_ref.at[pl.ds(i * share, share)]
        return pltpu.make_async_remote_copy(
            src_ref=block,
            dst_ref=block,
            send_sem=fin_send.at[dest],
            recv_sem=fin_recv.at[i],
            device_id={"seq": dest},
            device_id_type=MESH,
        )

    def iota(shape, dim):
        return lax.broadcasted_iota(jnp.int32, shape, dim)

    small[0].wait()
    small[1].wait()
    entry = iota((1, pool), 1)
    live = jnp.zeros((1, pool), jnp.int32)
    owner_seq = jnp.zeros((1, pool), jnp.int32)
    for b in range(batch):
        past = entry >= b * table_width
        left = jnp.clip(len_smem[b] - page * (entry - b * table_width), 0, page)
        live = jnp.where(past, left, live)
        owner_seq = jnp.where(past, b, owner_seq)
    hit = pt_vmem[...].reshape(1, pool) == me * slots + iota((slots, pool), 0)
    seq_col = jnp.sum(jnp.where(hit, owner_seq.astype(f32), 0.0), axis=1, keepdims=True)
    live_col = jnp.sum(jnp.where(hit, live.astype(f32), 0.0), axis=1, keepdims=True)
    seq_wide = jnp.broadcast_to(seq_col, (slots, page))
    slot_seq[...] = seq_wide
    slot_live[...] = jnp.broadcast_to(live_col, (slots, page))
    lane = iota((rows, page), 1)
    lane_f = lane.astype(f32)
    diagonal = iota((slots, page), 0) == iota((slots, page), 1)
    seq_row = jnp.sum(jnp.where(diagonal, seq_wide, 0.0), axis=0, keepdims=True)
    seq_row = jnp.where(iota((1, page), 1) < slots, seq_row, -1.0)
    row_vmem[...] = jnp.clip(seq_row.astype(jnp.int32), 0, batch - 1)
    row_copy = pltpu.make_async_copy(row_vmem, row_smem, small_sem.at[3])
    row_copy.start()
    seq_row = jnp.broadcast_to(seq_row, (rows, page))

    small[2].wait()
    column = iota((heads, 2 * batch * heads), 1)
    line = iota((heads, 2 * batch * heads), 0)
    side = column // (batch * heads) == line % rows // half
    mark = jnp.where((column % heads == line) & side, column % (batch * heads) // heads, -1)
    mark = mark.astype(f32)
    queries = q_raw[...].reshape(batch * heads, head_dim)
    blank = jnp.zeros_like(queries)
    queries = jnp.concatenate(
        [
            jnp.concatenate([queries, blank], axis=1),
            jnp.concatenate([blank, queries], axis=1),
        ],
        axis=0,
    )
    for unit in range(2):
        pltpu.matmul_push_rhs(queries, staging_register=0, mxu_index=unit)
    group = slots // len(pick_acc)
    for i, acc in enumerate(pick_acc):
        pick = []
        for pp in range(i * group // 2, (i + 1) * group // 2):
            for j in range(pairs):
                for p in (2 * pp, 2 * pp + 1):
                    seq = slot_seq[p : p + 1, :]
                    seq = jnp.concatenate([seq, seq], axis=1)
                    pick.append(jnp.where(mark[j * rows : (j + 1) * rows] == seq, 1.0, 0.0))
        pick = jnp.concatenate(pick, axis=0).astype(bf16)
        pltpu.matmul_acc_lhs(acc, pick, load_staged_rhs=0 if i < 2 else None)
    for i, acc in enumerate(pick_acc):
        picked[i * group * heads : (i + 1) * group * heads, :] = pltpu.matmul_pop(acc).astype(bf16)

    wide = (iota((batch * rows, page), 0) // rows).astype(f32)
    each = iota((batch, page), 0).astype(f32)
    peaks = {(j, b): jnp.full((rows, page), VERY_LOW, f32) for j in range(pairs) for b in range(batch)}
    sums = [jnp.zeros((rows, page), f32) for _ in range(pairs)]

    def prepare(p):
        choose[p] = jnp.where(wide == slot_seq[p : p + 1, :], 1.0, 0.0).astype(bf16)
        bias[p] = jnp.where(each == slot_seq[p : p + 1, :], 0.0, VERY_LOW)

    def score(pp, j):
        both = [
            k_vmem[2 * pp : 2 * pp + 2, 2 * j + g].reshape(2 * page, head_dim) for g in range(2)
        ]
        tile = pp * pairs + j
        register = tile // 2 % 2
        pltpu.matmul_push_rhs(
            jnp.concatenate(both, axis=1),
            staging_register=register,
            mxu_index=tile % 2,
            transpose=True,
        )
        pltpu.matmul_acc_lhs(
            score_acc[tile],
            picked[tile * 2 * rows : (tile + 1) * 2 * rows, :],
            load_staged_rhs=register,
        )

    def scores(pp, j):
        found = pltpu.matmul_pop(score_acc[pp * pairs + j])
        return [found[i * rows : (i + 1) * rows, i * page : (i + 1) * page] for i in range(2)]

    def settle(p, j, s):
        s = jnp.where(lane_f < slot_live[p : p + 1, :], s * factor, VERY_LOW)
        soft[p, j] = s
        for b in range(batch):
            peaks[j, b] = jnp.maximum(peaks[j, b], s + bias[p, b : b + 1, :])

    for i in range(KEY_PIECES + 1):
        if i < KEY_PIECES:
            k_copies[i].wait()
            if i >= VALUE_LEAD:
                unstarted.pop(0).start()
            for pp in range(i * span // 2, (i + 1) * span // 2):
                for j in range(pairs):
                    score(pp, j)
            for p in range(i * span, (i + 1) * span):
                prepare(p)
        if i > 0:
            for pp in range((i - 1) * span // 2, i * span // 2):
                for j in range(pairs):
                    for k, found in enumerate(scores(pp, j)):
                        settle(2 * pp + k, j, found)

    row_copy.wait()
    for copy in unstarted:
        copy.start()
    for key in peaks:
        j, b = key
        peaks[key] = jnp.maximum(jnp.max(peaks[key], axis=1, keepdims=True), FLOOR)
        crest[b, j] = jnp.broadcast_to(peaks[key], (rows, page))

    def soften(j, p):
        seq = jnp.clip(row_smem[0, p], 0, batch - 1)
        w = jnp.exp2(soft[p, j] - crest[seq, j])
        sums[j] = jnp.where(lane == p, jnp.sum(w, axis=1, keepdims=True), sums[j])
        w = jnp.concatenate([w] * 2, axis=0).astype(bf16)
        w = jnp.concatenate([w] * (batch // 2), axis=0)
        spread[j, :, p * page : (p + 1) * page] = w * choose[p]

    stats = [jnp.zeros((rows, page), f32) for _ in range(parts)]
    inverse = {}

    def account(j):
        for b in range(batch):
            total = jnp.where(seq_row == float(b), sums[j], 0.0)
            total = jnp.sum(total, axis=1, keepdims=True)
            some = total > 0.0
            safe = jnp.where(some, total, 1.0)
            level = jnp.where(some, peaks[j, b] + jnp.log2(safe), VERY_LOW)
            inverse[j, b] = jnp.broadcast_to(1.0 / safe, (rows, head_dim))
            i, local = b // share, b % share
            stats[i] = jnp.where(lane == j * share + local, level, stats[i])

    upper = iota((batch * rows, head_dim), 0) % rows < half

    def gather(j, at, size):
        for pp in range(at // 2, (at + size) // 2):
            both = [
                v_vmem[2 * pp : 2 * pp + 2, 2 * j + g].reshape(2 * page, head_dim)
                for g in range(2)
            ]
            register = pp // 2 % 2
            pltpu.matmul_push_rhs(
                jnp.concatenate(both, axis=1), staging_register=register, mxu_index=pp % 2
            )
            pltpu.matmul_acc_lhs(
                value_acc[2 * j + pp % 2],
                spread[j, :, 2 * pp * page : 2 * (pp + 1) * page],
                load_staged_rhs=register,
            )

    def merge(j):
        found = pltpu.matmul_pop(value_acc[2 * j]) + pltpu.matmul_pop(value_acc[2 * j + 1])
        return jnp.where(upper, found[:, :head_dim], found[:, head_dim:])

    def post_stats():
        for i in range(parts):
            stat_out[i] = stats[i]
        pl.semaphore_wait(barrier, jnp.where(mine, parts - 1, parts))
        for i, o in enumerate(owners):
            @pl.when(me != o)
            def _():
                stat_copy(i, me).start()

            @pl.when(me == o)
            def _():
                stat_in[me] = stat_out[i]

    def post_numer(j, numer):
        scale = jnp.concatenate([inverse[j, b] for b in range(batch)], axis=0)
        num_out[j] = (numer * scale).astype(bf16).reshape(parts, share * rows, head_dim)
        for i, o in enumerate(owners):
            @pl.when(me != o)
            def _():
                num_copy(j, i, me).start()

            @pl.when(me == o)
            def _():
                num_in[j, me] = num_out[j, i]

    for p in range(slots):
        soften(0, p)
    owed = None
    for j, at, size, copy in v_copies:
        copy.wait()
        gather(j, at, size)
        if j == 0:
            if at == 0:
                account(0)
            for other in range(1, pairs):
                for p in range(at, at + size):
                    soften(other, p)
            if at + size == slots:
                for other in range(1, pairs):
                    account(other)
        if owed is not None:
            if owed == 0:
                post_stats()
            post_numer(owed, merge(owed))
        owed = j if at + size == slots else None
    post_numer(owed, merge(owed))

    @pl.when(mine)
    def _():
        for step in range(1, n):
            stat_copy(0, lax.rem(me + step, n)).wait_recv()
        levels = stat_in[...]
        scales = jnp.exp2(levels - jnp.max(levels, axis=0, keepdims=True))
        scales = scales / jnp.sum(scales, axis=0, keepdims=True)
        columns = {}
        for s in range(n):
            for at in range(pairs * share):
                columns[s, at] = jnp.broadcast_to(scales[s][:, at : at + 1], (rows, head_dim))
        blocks = []
        for j in range(pairs):
            for step in range(1, n):
                num_copy(j, 0, lax.rem(me + step, n)).wait_recv()
            for local in range(share):
                blocks.append(
                    sum(
                        columns[s, j * share + local]
                        * num_in[j, s, local * rows : (local + 1) * rows, :].astype(f32)
                        for s in range(n)
                    )
                )
        for local in range(share):
            whole = [blocks[j * share + local] for j in range(pairs)]
            out_ref[rank * share + local] = jnp.concatenate(whole, axis=0).astype(out_ref.dtype)
        for step in range(1, n):
            fin_copy(lax.rem(me + step, n), rank).start()

    for i, o in enumerate(owners):
        @pl.when(me != o)
        def _():
            stat_copy(i, me).wait_send()
            for j in range(pairs):
                num_copy(j, i, me).wait_send()
            fin_copy(o, i).wait_recv()

    @pl.when(mine)
    def _():
        for step in range(1, n):
            fin_copy(lax.rem(me + step, n), rank).wait_send()


def scoped(n, table_width, owners, batch, heads, slots, pairs, *refs):
    rows = heads // pairs
    pieces = 4
    accs = []
    for i in range(pieces):
        accs.append(pltpu.ACC(i % 2)((slots * heads // pieces, 256), jnp.float32))
    tiles = slots // 2 * pairs
    for i in range(tiles):
        accs.append(pltpu.ACC(i % 2)((2 * rows, 256), jnp.float32))
    for i in range(2 * pairs):
        accs.append(pltpu.ACC(i % 2)((batch * rows, 256), jnp.float32))

    def body(*accs):
        attend(
            n,
            table_width,
            owners,
            accs[:pieces],
            accs[pieces : pieces + tiles],
            accs[pieces + tiles :],
            *refs,
        )

    pl.run_scoped(body, *accs)


def shards(n, owners, query_rows, cache_keys, cache_values, page_table, seq_lengths):
    slots, kv_heads, page, head_dim = cache_keys.shape
    batch, heads, _ = query_rows.shape
    pool = page_table.shape[0]
    rows, pairs = 2 * heads // kv_heads, kv_heads // 2
    parts = len(owners)
    share = batch // parts
    f32, bf16 = jnp.float32, jnp.bfloat16
    hbm = pl.BlockSpec(memory_space=pl.ANY)
    dma = pltpu.SemaphoreType.DMA
    return pl.pallas_call(
        functools.partial(scoped, n, pool // batch, owners, batch, heads, slots, pairs),
        out_shape=pltpu.VMEM((batch, heads, head_dim), bf16),
        in_specs=[hbm] * 5,
        out_specs=pl.BlockSpec(memory_space=pltpu.VMEM),
        scratch_shapes=[
            pltpu.VMEM((batch, heads, head_dim), bf16),
            pltpu.VMEM((pool,), jnp.int32),
            pltpu.SMEM((batch,), jnp.int32),
            pltpu.VMEM((slots, kv_heads, page, head_dim), bf16),
            pltpu.VMEM((slots, kv_heads, page, head_dim), bf16),
            pltpu.VMEM((slots, page), f32),
            pltpu.VMEM((slots, page), f32),
            pltpu.VMEM((slots * heads, 2 * head_dim), bf16),
            pltpu.VMEM((slots, batch * rows, page), bf16),
            pltpu.VMEM((slots, pairs, rows, page), f32),
            pltpu.VMEM((pairs, batch * rows, slots * page), bf16),
            pltpu.VMEM((slots, batch, page), f32),
            pltpu.VMEM((batch, pairs, rows, page), f32),
            pltpu.VMEM((1, page), jnp.int32),
            pltpu.SMEM((1, page), jnp.int32),
            pltpu.VMEM((parts, rows, page), f32),
            pltpu.VMEM((n, rows, page), f32),
            pltpu.VMEM((pairs, parts, share * rows, head_dim), bf16),
            pltpu.VMEM((pairs, n, share * rows, head_dim), bf16),
            dma((4,)),
            dma((KEY_PIECES,)),
            dma((sum(len(VALUE_PIECES[min(j, 1)]) for j in range(pairs)),)),
            dma((parts,)),
            dma((n,)),
            dma((pairs, parts)),
            dma((pairs, n)),
            dma((n,)),
            dma((parts,)),
        ],
        compiler_params=pltpu.CompilerParams(collective_id=0, has_side_effects=True),
    )(query_rows, cache_keys, cache_values, page_table, seq_lengths)


def owners_of(n):
    return tuple(range(4))


def solution(mesh):
    n = mesh.shape["seq"]
    owners = owners_of(n)
    in_specs = (
        P("grp", "head", None),
        P(("grp", "seq"), "head", None, None),
        P(("grp", "seq"), "head", None, None),
        P("grp"),
        P("grp"),
    )
    return jax.shard_map(
        functools.partial(shards, n, owners),
        mesh=mesh,
        in_specs=in_specs,
        out_specs=P("grp", "head", None),
        check_vma=False,
    )
```

```python
import functools
import math

import jax
import jax.numpy as jnp
from jax import lax
from jax.experimental import pallas as pl
from jax.experimental.pallas import tpu as pltpu
from jax.sharding import PartitionSpec as P

MESH = pl.DeviceIdType.MESH
VERY_LOW = -1e30
FLOOR = -1e29
KEY_PIECES = 8
VALUE_PIECES = ((1, 1, 1, 1), (2, 2, 2, 1, 1))
EARLY = 1
STEP = 1
PAUSE = 100


def attend(
    n,
    sides,
    table_width,
    owners,
    pick_acc,
    score_acc,
    value_acc,
    q_hbm,
    k_hbm,
    v_hbm,
    pt_hbm,
    len_hbm,
    out_ref,
    q_raw,
    pt_vmem,
    len_smem,
    k_vmem,
    v_vmem,
    slot_seq,
    slot_live,
    picked,
    choose,
    soft,
    spread,
    bias,
    crest,
    row_vmem,
    row_smem,
    done_ref,
    stat_out,
    stat_in,
    num_out,
    num_in,
    small_sem,
    k_sem,
    v_sem,
    stat_send,
    stat_recv,
    num_send,
    num_recv,
    fin_send,
    fin_recv,
):
    me = lax.axis_index("seq")
    side = lax.axis_index("head")
    gate = sides - 1
    slot = side * n + me
    batch, heads, head_dim = q_raw.shape
    slots, kv_heads, page, _ = k_vmem.shape
    pairs = kv_heads // 2
    half = heads // kv_heads
    rows = 2 * half
    pool = pt_vmem.shape[0]
    parts = len(owners)
    share = batch // parts
    f32, bf16 = jnp.float32, jnp.bfloat16
    factor = math.log2(math.e) / math.sqrt(head_dim)

    small = (
        pltpu.make_async_copy(pt_hbm, pt_vmem, small_sem.at[0]),
        pltpu.make_async_copy(len_hbm, len_smem, small_sem.at[1]),
        pltpu.make_async_copy(q_hbm, q_raw, small_sem.at[2]),
    )
    for copy in small:
        copy.start()
    pl.delay(PAUSE)
    span = slots // KEY_PIECES
    k_copies = [
        pltpu.make_async_copy(
            k_hbm.at[pl.ds(i * span, span)], k_vmem.at[pl.ds(i * span, span)], k_sem.at[i]
        )
        for i in range(KEY_PIECES)
    ]
    v_copies = []
    for j in range(pairs):
        cuts = VALUE_PIECES[min(j, 1)]
        unit, at = slots // sum(cuts), 0
        for size in cuts:
            pages = pl.ds(at, size * unit)
            v_copies.append(
                (
                    j,
                    at,
                    size * unit,
                    pltpu.make_async_copy(
                        v_hbm.at[pages, pl.ds(2 * j, 2)],
                        v_vmem.at[pages, pl.ds(2 * j, 2)],
                        v_sem.at[len(v_copies)],
                    ),
                )
            )
            at += size * unit
    for copy in k_copies:
        copy.start()
    unstarted = [copy for _, _, _, copy in v_copies]
    for _ in range(EARLY):
        unstarted.pop(0).start()

    mine = (side == gate) & functools.reduce(lambda a, b: a | b, [me == o for o in owners])
    rank = sum(jnp.where(me == o, i, 0) for i, o in enumerate(owners))
    barrier = pltpu.get_barrier_semaphore()

    def others():
        for h in range(sides):
            for step in range(1 if h == gate else 0, n):
                yield h, lax.rem(me + step, n)

    @pl.when(mine)
    def _():
        for h, seq in others():
            pl.semaphore_signal(
                barrier, inc=1, device_id={"seq": seq, "head": h}, device_id_type=MESH
            )

    def stat_copy(i, slot):
        return pltpu.make_async_remote_copy(
            src_ref=stat_out.at[i],
            dst_ref=stat_in.at[slot],
            send_sem=stat_send.at[i],
            recv_sem=stat_recv.at[slot],
            device_id={"seq": owners[i], "head": gate},
            device_id_type=MESH,
        )

    def num_copy(j, i, slot):
        return pltpu.make_async_remote_copy(
            src_ref=num_out.at[j, i],
            dst_ref=num_in.at[j, slot],
            send_sem=num_send.at[j, i],
            recv_sem=num_recv.at[j, slot],
            device_id={"seq": owners[i], "head": gate},
            device_id_type=MESH,
        )

    def fin_copy(h, seq, i):
        return pltpu.make_async_remote_copy(
            src_ref=done_ref.at[h],
            dst_ref=out_ref.at[pl.ds(i * share, share)],
            send_sem=fin_send.at[h, seq],
            recv_sem=fin_recv.at[i],
            device_id={"seq": seq, "head": h},
            device_id_type=MESH,
        )

    def own(o):
        return (me == o) & (side == gate)

    def foreign(o):
        return (me != o) | (side != gate)

    def iota(shape, dim):
        return lax.broadcasted_iota(jnp.int32, shape, dim)

    small[0].wait()
    small[1].wait()
    entry = iota((1, pool), 1)
    live = jnp.zeros((1, pool), jnp.int32)
    owner_seq = jnp.zeros((1, pool), jnp.int32)
    for b in range(batch):
        past = entry >= b * table_width
        left = jnp.clip(len_smem[b] - page * (entry - b * table_width), 0, page)
        live = jnp.where(past, left, live)
        owner_seq = jnp.where(past, b, owner_seq)
    hit = pt_vmem[...].reshape(1, pool) == me * slots + iota((slots, pool), 0)
    seq_col = jnp.sum(jnp.where(hit, owner_seq.astype(f32), 0.0), axis=1, keepdims=True)
    live_col = jnp.sum(jnp.where(hit, live.astype(f32), 0.0), axis=1, keepdims=True)
    seq_wide = jnp.broadcast_to(seq_col, (slots, page))
    slot_seq[...] = seq_wide
    slot_live[...] = jnp.broadcast_to(live_col, (slots, page))
    lane = iota((rows, page), 1)
    lane_f = lane.astype(f32)
    diagonal = iota((slots, page), 0) == iota((slots, page), 1)
    seq_row = jnp.sum(jnp.where(diagonal, seq_wide, 0.0), axis=0, keepdims=True)
    seq_row = jnp.where(iota((1, page), 1) < slots, seq_row, -1.0)
    row_vmem[...] = jnp.clip(seq_row.astype(jnp.int32), 0, batch - 1)
    row_copy = pltpu.make_async_copy(row_vmem, row_smem, small_sem.at[3])
    row_copy.start()
    seq_row = jnp.broadcast_to(seq_row, (rows, page))

    small[2].wait()
    column = iota((heads, 2 * batch * heads), 1)
    line = iota((heads, 2 * batch * heads), 0)
    match = column // (batch * heads) == line % rows // half
    mark = jnp.where((column % heads == line) & match, column % (batch * heads) // heads, -1)
    mark = mark.astype(f32)
    queries = q_raw[...].reshape(batch * heads, head_dim)
    blank = jnp.zeros_like(queries)
    queries = jnp.concatenate(
        [
            jnp.concatenate([queries, blank], axis=1),
            jnp.concatenate([blank, queries], axis=1),
        ],
        axis=0,
    )
    for unit in range(2):
        pltpu.matmul_push_rhs(queries, staging_register=0, mxu_index=unit)
    group = slots // len(pick_acc)
    for i, acc in enumerate(pick_acc):
        pick = []
        for pp in range(i * group // 2, (i + 1) * group // 2):
            for j in range(pairs):
                for p in (2 * pp, 2 * pp + 1):
                    seq = slot_seq[p : p + 1, :]
                    seq = jnp.concatenate([seq, seq], axis=1)
                    pick.append(jnp.where(mark[j * rows : (j + 1) * rows] == seq, 1.0, 0.0))
        pick = jnp.concatenate(pick, axis=0).astype(bf16)
        pltpu.matmul_acc_lhs(acc, pick, load_staged_rhs=0 if i < 2 else None)
    for i, acc in enumerate(pick_acc):
        picked[i * group * heads : (i + 1) * group * heads, :] = pltpu.matmul_pop(acc).astype(bf16)

    wide = (iota((batch * rows, page), 0) // rows).astype(f32)
    each = iota((batch, page), 0).astype(f32)
    peaks = {(j, b): jnp.full((rows, page), VERY_LOW, f32) for j in range(pairs) for b in range(batch)}
    sums = [jnp.zeros((rows, page), f32) for _ in range(pairs)]

    def prepare(p):
        choose[p] = jnp.where(wide == slot_seq[p : p + 1, :], 1.0, 0.0).astype(bf16)
        bias[p] = jnp.where(each == slot_seq[p : p + 1, :], 0.0, VERY_LOW)

    def score(pp, j):
        both = [
            k_vmem[2 * pp : 2 * pp + 2, 2 * j + g].reshape(2 * page, head_dim) for g in range(2)
        ]
        tile = pp * pairs + j
        register = tile // 2 % 2
        pltpu.matmul_push_rhs(
            jnp.concatenate(both, axis=1),
            staging_register=register,
            mxu_index=tile % 2,
            transpose=True,
        )
        pltpu.matmul_acc_lhs(
            score_acc[tile],
            picked[tile * 2 * rows : (tile + 1) * 2 * rows, :],
            load_staged_rhs=register,
        )

    def scores(pp, j):
        found = pltpu.matmul_pop(score_acc[pp * pairs + j])
        return [found[i * rows : (i + 1) * rows, i * page : (i + 1) * page] for i in range(2)]

    def settle(p, j, s):
        s = jnp.where(lane_f < slot_live[p : p + 1, :], s * factor, VERY_LOW)
        soft[p, j] = s
        for b in range(batch):
            peaks[j, b] = jnp.maximum(peaks[j, b], s + bias[p, b : b + 1, :])

    for i in range(KEY_PIECES + 1):
        if i < KEY_PIECES:
            k_copies[i].wait()
            for _ in range(min(STEP, len(unstarted))):
                unstarted.pop(0).start()
            for pp in range(i * span // 2, (i + 1) * span // 2):
                for j in range(pairs):
                    score(pp, j)
            for p in range(i * span, (i + 1) * span):
                prepare(p)
        if i > 0:
            for pp in range((i - 1) * span // 2, i * span // 2):
                for j in range(pairs):
                    for k, found in enumerate(scores(pp, j)):
                        settle(2 * pp + k, j, found)

    row_copy.wait()
    for copy in unstarted:
        copy.start()
    for key in peaks:
        j, b = key
        peaks[key] = jnp.maximum(jnp.max(peaks[key], axis=1, keepdims=True), FLOOR)
        crest[b, j] = jnp.broadcast_to(peaks[key], (rows, page))

    def soften(j, p):
        seq = jnp.clip(row_smem[0, p], 0, batch - 1)
        w = jnp.exp2(soft[p, j] - crest[seq, j])
        sums[j] = jnp.where(lane == p, jnp.sum(w, axis=1, keepdims=True), sums[j])
        w = jnp.concatenate([w] * 2, axis=0).astype(bf16)
        w = jnp.concatenate([w] * (batch // 2), axis=0)
        spread[j, :, p * page : (p + 1) * page] = w * choose[p]

    stats = [jnp.zeros((rows, page), f32) for _ in range(parts)]
    inverse = {}

    def account(j):
        for b in range(batch):
            total = jnp.where(seq_row == float(b), sums[j], 0.0)
            total = jnp.sum(total, axis=1, keepdims=True)
            some = total > 0.0
            safe = jnp.where(some, total, 1.0)
            level = jnp.where(some, peaks[j, b] + jnp.log2(safe), VERY_LOW)
            inverse[j, b] = jnp.broadcast_to(1.0 / safe, (rows, head_dim))
            i, local = b // share, b % share
            stats[i] = jnp.where(lane == j * share + local, level, stats[i])

    upper = iota((batch * rows, head_dim), 0) % rows < half

    def gather(j, at, size):
        for pp in range(at // 2, (at + size) // 2):
            both = [
                v_vmem[2 * pp : 2 * pp + 2, 2 * j + g].reshape(2 * page, head_dim)
                for g in range(2)
            ]
            register = pp // 2 % 2
            pltpu.matmul_push_rhs(
                jnp.concatenate(both, axis=1), staging_register=register, mxu_index=pp % 2
            )
            pltpu.matmul_acc_lhs(
                value_acc[2 * j + pp % 2],
                spread[j, :, 2 * pp * page : 2 * (pp + 1) * page],
                load_staged_rhs=register,
            )

    def merge(j):
        found = pltpu.matmul_pop(value_acc[2 * j]) + pltpu.matmul_pop(value_acc[2 * j + 1])
        return jnp.where(upper, found[:, :head_dim], found[:, head_dim:])

    def post_stats():
        for i in range(parts):
            stat_out[i] = stats[i]
        pl.semaphore_wait(barrier, jnp.where(mine, parts - 1, parts))
        for i, o in enumerate(owners):
            @pl.when(foreign(o))
            def _():
                stat_copy(i, slot).start()

            @pl.when(own(o))
            def _():
                stat_in[slot] = stat_out[i]

    def post_numer(j, numer):
        scale = jnp.concatenate([inverse[j, b] for b in range(batch)], axis=0)
        num_out[j] = (numer * scale).reshape(parts, share * rows, head_dim)
        for i, o in enumerate(owners):
            @pl.when(foreign(o))
            def _():
                num_copy(j, i, slot).start()

            @pl.when(own(o))
            def _():
                num_in[j, slot] = num_out[j, i]

    for p in range(slots):
        soften(0, p)
    owed = None
    for j, at, size, copy in v_copies:
        copy.wait()
        gather(j, at, size)
        if j == 0:
            if at == 0:
                account(0)
            for other in range(1, pairs):
                for p in range(at, at + size):
                    soften(other, p)
            if at + size == slots:
                for other in range(1, pairs):
                    account(other)
        if owed is not None:
            if owed == 0:
                post_stats()
            post_numer(owed, merge(owed))
        owed = j if at + size == slots else None
    post_numer(owed, merge(owed))

    @pl.when(mine)
    def _():
        columns = {}
        for h in range(sides):
            for other, seq in others():
                if other == h:
                    stat_copy(0, h * n + seq).wait_recv()
            levels = stat_in[h * n : (h + 1) * n]
            scales = jnp.exp2(levels - jnp.max(levels, axis=0, keepdims=True))
            scales = scales / jnp.sum(scales, axis=0, keepdims=True)
            for s in range(n):
                for at in range(pairs * share):
                    columns[h, s, at] = jnp.broadcast_to(
                        scales[s][:, at : at + 1], (rows, head_dim)
                    )
        for h in range(sides):
            blocks = []
            for j in range(pairs):
                for other, seq in others():
                    if other == h:
                        num_copy(j, 0, h * n + seq).wait_recv()
                for local in range(share):
                    blocks.append(
                        sum(
                            columns[h, s, j * share + local]
                            * num_in[j, h * n + s, local * rows : (local + 1) * rows, :]
                            for s in range(n)
                        )
                    )
            for local in range(share):
                whole = [blocks[j * share + local] for j in range(pairs)]
                whole = jnp.concatenate(whole, axis=0).astype(out_ref.dtype)
                done_ref[h, local] = whole
                if h == gate:
                    out_ref[rank * share + local] = whole
            for other, seq in others():
                if other == h:
                    fin_copy(h, seq, rank).start()

    for i, o in enumerate(owners):
        @pl.when(foreign(o))
        def _():
            stat_copy(i, slot).wait_send()
            for j in range(pairs):
                num_copy(j, i, slot).wait_send()
            fin_copy(0, o, i).wait_recv()

    @pl.when(mine)
    def _():
        for h, seq in others():
            fin_copy(h, seq, rank).wait_send()


def scoped(n, sides, table_width, owners, batch, heads, slots, pairs, *refs):
    rows = heads // pairs
    pieces = 4
    accs = []
    for i in range(pieces):
        accs.append(pltpu.ACC(i % 2)((slots * heads // pieces, 256), jnp.float32))
    tiles = slots // 2 * pairs
    for i in range(tiles):
        accs.append(pltpu.ACC(i % 2)((2 * rows, 256), jnp.float32))
    for i in range(2 * pairs):
        accs.append(pltpu.ACC(i % 2)((batch * rows, 256), jnp.float32))

    def body(*accs):
        attend(
            n,
            sides,
            table_width,
            owners,
            accs[:pieces],
            accs[pieces : pieces + tiles],
            accs[pieces + tiles :],
            *refs,
        )

    pl.run_scoped(body, *accs)


def shards(n, sides, owners, query_rows, cache_keys, cache_values, page_table, seq_lengths):
    slots, kv_heads, page, head_dim = cache_keys.shape
    batch, heads, _ = query_rows.shape
    pool = page_table.shape[0]
    rows, pairs = 2 * heads // kv_heads, kv_heads // 2
    parts = len(owners)
    share = batch // parts
    f32, bf16 = jnp.float32, jnp.bfloat16
    hbm = pl.BlockSpec(memory_space=pl.ANY)
    dma = pltpu.SemaphoreType.DMA
    return pl.pallas_call(
        functools.partial(scoped, n, sides, pool // batch, owners, batch, heads, slots, pairs),
        out_shape=pltpu.VMEM((batch, heads, head_dim), bf16),
        in_specs=[hbm] * 5,
        out_specs=pl.BlockSpec(memory_space=pltpu.VMEM),
        scratch_shapes=[
            pltpu.VMEM((batch, heads, head_dim), bf16),
            pltpu.VMEM((pool,), jnp.int32),
            pltpu.SMEM((batch,), jnp.int32),
            pltpu.VMEM((slots, kv_heads, page, head_dim), bf16),
            pltpu.VMEM((slots, kv_heads, page, head_dim), bf16),
            pltpu.VMEM((slots, page), f32),
            pltpu.VMEM((slots, page), f32),
            pltpu.VMEM((slots * heads, 2 * head_dim), bf16),
            pltpu.VMEM((slots, batch * rows, page), bf16),
            pltpu.VMEM((slots, pairs, rows, page), f32),
            pltpu.VMEM((pairs, batch * rows, slots * page), bf16),
            pltpu.VMEM((slots, batch, page), f32),
            pltpu.VMEM((batch, pairs, rows, page), f32),
            pltpu.VMEM((1, page), jnp.int32),
            pltpu.SMEM((1, page), jnp.int32),
            pltpu.VMEM((sides, share, heads, head_dim), bf16),
            pltpu.VMEM((parts, rows, page), f32),
            pltpu.VMEM((sides * n, rows, page), f32),
            pltpu.VMEM((pairs, parts, share * rows, head_dim), f32),
            pltpu.VMEM((pairs, sides * n, share * rows, head_dim), f32),
            dma((4,)),
            dma((KEY_PIECES,)),
            dma((sum(len(VALUE_PIECES[min(j, 1)]) for j in range(pairs)),)),
            dma((parts,)),
            dma((sides * n,)),
            dma((pairs, parts)),
            dma((pairs, sides * n)),
            dma((sides, n)),
            dma((parts,)),
        ],
        compiler_params=pltpu.CompilerParams(collective_id=0, has_side_effects=True),
    )(query_rows, cache_keys, cache_values, page_table, seq_lengths)


def owners_of(n):
    return tuple(range(n // 2 - 2, n // 2 + 2))


def solution(mesh):
    n = mesh.shape["seq"]
    owners = owners_of(n)
    in_specs = (
        P("grp", "head", None),
        P(("grp", "seq"), "head", None, None),
        P(("grp", "seq"), "head", None, None),
        P("grp"),
        P("grp"),
    )
    return jax.shard_map(
        functools.partial(shards, n, mesh.shape["head"], owners),
        mesh=mesh,
        in_specs=in_specs,
        out_specs=P("grp", "head", None),
        check_vma=False,
    )
```

```python
import functools
import math

import jax
import jax.numpy as jnp
from jax import lax
from jax.experimental import pallas as pl
from jax.experimental.pallas import tpu as pltpu
from jax.sharding import PartitionSpec as P

MESH = pl.DeviceIdType.MESH
VERY_LOW = -1e30
FLOOR = -1e29
KEY_PIECES = 8
VALUE_PIECES = ((1, 1, 1, 1), (2, 2, 2, 1, 1))
EARLY = 1
STEP = 1
PAUSE = 100


def attend(
    n,
    sides,
    table_width,
    owners,
    pick_acc,
    score_acc,
    value_acc,
    q_hbm,
    k_hbm,
    v_hbm,
    pt_hbm,
    len_hbm,
    out_ref,
    q_raw,
    pt_vmem,
    len_smem,
    k_vmem,
    v_vmem,
    slot_seq,
    slot_live,
    picked,
    choose,
    soft,
    spread,
    bias,
    crest,
    row_vmem,
    row_smem,
    done_ref,
    tally,
    stat_out,
    stat_in,
    num_out,
    num_in,
    small_sem,
    k_sem,
    v_sem,
    stat_send,
    stat_recv,
    num_send,
    num_recv,
    fin_send,
    fin_recv,
):
    me = lax.axis_index("seq")
    side = lax.axis_index("head")
    gate = sides - 1
    slot = side * n + me
    batch, heads, head_dim = q_raw.shape
    slots, kv_heads, page, _ = k_vmem.shape
    pairs = kv_heads // 2
    half = heads // kv_heads
    rows = 2 * half
    pool = pt_vmem.shape[0]
    parts = len(owners)
    share = batch // parts
    f32, bf16 = jnp.float32, jnp.bfloat16
    factor = math.log2(math.e) / math.sqrt(head_dim)

    small = (
        pltpu.make_async_copy(pt_hbm, pt_vmem, small_sem.at[0]),
        pltpu.make_async_copy(len_hbm, len_smem, small_sem.at[1]),
        pltpu.make_async_copy(q_hbm, q_raw, small_sem.at[2]),
    )
    for copy in small:
        copy.start()
    pl.delay(PAUSE)
    span = slots // KEY_PIECES
    k_copies = [
        pltpu.make_async_copy(
            k_hbm.at[pl.ds(i * span, span)], k_vmem.at[pl.ds(i * span, span)], k_sem.at[i]
        )
        for i in range(KEY_PIECES)
    ]
    v_copies = []
    for j in range(pairs):
        cuts = VALUE_PIECES[min(j, 1)]
        unit, at = slots // sum(cuts), 0
        for size in cuts:
            pages = pl.ds(at, size * unit)
            v_copies.append(
                (
                    j,
                    at,
                    size * unit,
                    pltpu.make_async_copy(
                        v_hbm.at[pages, pl.ds(2 * j, 2)],
                        v_vmem.at[pages, pl.ds(2 * j, 2)],
                        v_sem.at[len(v_copies)]
                        if len(v_copies) < EARLY
                        else k_sem.at[len(v_copies) - EARLY],
                    ),
                )
            )
            at += size * unit
    for copy in k_copies:
        copy.start()
    unstarted = [copy for _, _, _, copy in v_copies]
    for _ in range(EARLY):
        unstarted.pop(0).start()

    mine = (side == gate) & functools.reduce(lambda a, b: a | b, [me == o for o in owners])
    rank = sum(jnp.where(me == o, i, 0) for i, o in enumerate(owners))
    barrier = pltpu.get_barrier_semaphore()

    def others():
        for h in range(sides):
            for step in range(1 if h == gate else 0, n):
                yield h, lax.rem(me + step, n)

    @pl.when(mine)
    def _():
        for h, seq in others():
            pl.semaphore_signal(
                barrier, inc=1, device_id={"seq": seq, "head": h}, device_id_type=MESH
            )

    def stat_copy(i):
        return pltpu.make_async_remote_copy(
            src_ref=stat_out.at[i],
            dst_ref=stat_in.at[slot],
            send_sem=stat_send,
            recv_sem=stat_recv.at[side],
            device_id={"seq": owners[i], "head": gate},
            device_id_type=MESH,
        )

    def num_copy(j, i):
        return pltpu.make_async_remote_copy(
            src_ref=num_out.at[j, i],
            dst_ref=num_in.at[j, slot],
            send_sem=num_send,
            recv_sem=num_recv.at[j, side],
            device_id={"seq": owners[i], "head": gate},
            device_id_type=MESH,
        )

    def fin_copy(h, seq, i):
        return pltpu.make_async_remote_copy(
            src_ref=done_ref.at[h],
            dst_ref=out_ref.at[pl.ds(i * share, share)],
            send_sem=fin_send,
            recv_sem=fin_recv,
            device_id={"seq": seq, "head": h},
            device_id_type=MESH,
        )

    def bytes_of(ref, sem):
        return pltpu.make_async_remote_copy(
            src_ref=ref,
            dst_ref=ref,
            send_sem=sem,
            recv_sem=sem,
            device_id={"seq": owners[0], "head": gate},
            device_id_type=MESH,
        )

    def own(o):
        return (me == o) & (side == gate)

    def iota(shape, dim):
        return lax.broadcasted_iota(jnp.int32, shape, dim)

    small[0].wait()
    small[1].wait()
    entry = iota((1, pool), 1)
    live = jnp.zeros((1, pool), jnp.int32)
    owner_seq = jnp.zeros((1, pool), jnp.int32)
    for b in range(batch):
        past = entry >= b * table_width
        left = jnp.clip(len_smem[b] - page * (entry - b * table_width), 0, page)
        live = jnp.where(past, left, live)
        owner_seq = jnp.where(past, b, owner_seq)
    hit = pt_vmem[...].reshape(1, pool) == me * slots + iota((slots, pool), 0)
    seq_col = jnp.sum(jnp.where(hit, owner_seq.astype(f32), 0.0), axis=1, keepdims=True)
    live_col = jnp.sum(jnp.where(hit, live.astype(f32), 0.0), axis=1, keepdims=True)
    seq_wide = jnp.broadcast_to(seq_col, (slots, page))
    slot_seq[...] = seq_wide
    slot_live[...] = jnp.broadcast_to(live_col, (slots, page))
    lane = iota((rows, page), 1)
    lane_f = lane.astype(f32)
    diagonal = iota((slots, page), 0) == iota((slots, page), 1)
    seq_row = jnp.sum(jnp.where(diagonal, seq_wide, 0.0), axis=0, keepdims=True)
    seq_row = jnp.where(iota((1, page), 1) < slots, seq_row, -1.0)
    row_vmem[...] = jnp.clip(seq_row.astype(jnp.int32), 0, batch - 1)
    row_copy = pltpu.make_async_copy(row_vmem, row_smem, small_sem.at[0])
    row_copy.start()
    seq_row = jnp.broadcast_to(seq_row, (rows, page))

    small[2].wait()
    column = iota((heads, 2 * batch * heads), 1)
    line = iota((heads, 2 * batch * heads), 0)
    match = column // (batch * heads) == line % rows // half
    mark = jnp.where((column % heads == line) & match, column % (batch * heads) // heads, -1)
    mark = mark.astype(f32)
    queries = q_raw[...].reshape(batch * heads, head_dim)
    blank = jnp.zeros_like(queries)
    queries = jnp.concatenate(
        [
            jnp.concatenate([queries, blank], axis=1),
            jnp.concatenate([blank, queries], axis=1),
        ],
        axis=0,
    )
    for unit in range(2):
        pltpu.matmul_push_rhs(queries, staging_register=0, mxu_index=unit)
    group = slots // len(pick_acc)
    for i, acc in enumerate(pick_acc):
        pick = []
        for pp in range(i * group // 2, (i + 1) * group // 2):
            for j in range(pairs):
                for p in (2 * pp, 2 * pp + 1):
                    seq = slot_seq[p : p + 1, :]
                    seq = jnp.concatenate([seq, seq], axis=1)
                    pick.append(jnp.where(mark[j * rows : (j + 1) * rows] == seq, 1.0, 0.0))
        pick = jnp.concatenate(pick, axis=0).astype(bf16)
        pltpu.matmul_acc_lhs(acc, pick, load_staged_rhs=0 if i < 2 else None)
    def store_picks(i):
        found = pltpu.matmul_pop(pick_acc[i]).astype(bf16)
        here = pl.ds(i * group * heads, group * heads)
        picked[0, here] = found[:, :head_dim]
        picked[1, here] = found[:, head_dim:]

    store_picks(0)
    wide = (iota((batch * rows, page), 0) // rows).astype(f32)
    each = iota((batch, page), 0).astype(f32)
    peaks = {(j, b): jnp.full((rows, page), VERY_LOW, f32) for j in range(pairs) for b in range(batch)}
    sums = [jnp.zeros((rows, page), f32) for _ in range(pairs)]

    def prepare(p):
        choose[p] = jnp.where(wide == slot_seq[p : p + 1, :], 1.0, 0.0).astype(bf16)
        bias[p] = jnp.where(each == slot_seq[p : p + 1, :], 0.0, VERY_LOW)

    def score(pp, j):
        both = [
            k_vmem[2 * pp : 2 * pp + 2, 2 * j + g].reshape(2 * page, head_dim) for g in range(2)
        ]
        tile = pp * pairs + j
        register = tile // 2 % 2
        pltpu.matmul_push_rhs(
            jnp.concatenate(both, axis=1),
            staging_register=register,
            mxu_index=tile % 2,
            transpose=True,
        )
        pltpu.matmul_acc_lhs(
            score_acc[tile],
            jnp.concatenate([picked[g, pl.ds(tile * 2 * rows, 2 * rows)] for g in range(2)], axis=1),
            load_staged_rhs=register,
        )

    def scores(pp, j):
        found = pltpu.matmul_pop(score_acc[pp * pairs + j])
        return [found[i * rows : (i + 1) * rows, i * page : (i + 1) * page] for i in range(2)]

    def settle(p, j, s):
        s = jnp.where(lane_f < slot_live[p : p + 1, :], s * factor, VERY_LOW)
        soft[p, j] = s
        for b in range(batch):
            peaks[j, b] = jnp.maximum(peaks[j, b], s + bias[p, b : b + 1, :])

    for i in range(KEY_PIECES + 1):
        if i < KEY_PIECES:
            k_copies[i].wait()
            for _ in range(min(STEP, len(unstarted))):
                unstarted.pop(0).start()
            for pp in range(i * span // 2, (i + 1) * span // 2):
                for j in range(pairs):
                    score(pp, j)
            if i + 1 < KEY_PIECES:
                store_picks(i + 1)
            for p in range(i * span, (i + 1) * span):
                prepare(p)
        if i > 0:
            for pp in range((i - 1) * span // 2, i * span // 2):
                for j in range(pairs):
                    for k, found in enumerate(scores(pp, j)):
                        settle(2 * pp + k, j, found)

    row_copy.wait()
    for copy in unstarted:
        copy.start()
    for key in peaks:
        j, b = key
        peaks[key] = jnp.maximum(jnp.max(peaks[key], axis=1, keepdims=True), FLOOR)
        crest[b, j] = jnp.broadcast_to(peaks[key], (rows, page))

    def soften(j, p):
        seq = jnp.clip(row_smem[0, p], 0, batch - 1)
        w = jnp.exp2(soft[p, j] - crest[seq, j])
        sums[j] = jnp.where(lane == p, jnp.sum(w, axis=1, keepdims=True), sums[j])
        w = jnp.concatenate([w] * 2, axis=0).astype(bf16)
        w = jnp.concatenate([w] * (batch // 2), axis=0)
        spread[j, p] = w * choose[p]

    stats = [jnp.zeros((rows, page), f32) for _ in range(parts)]
    inverse = {}

    def account(j):
        for b in range(batch):
            total = jnp.where(seq_row == float(b), sums[j], 0.0)
            total = jnp.sum(total, axis=1, keepdims=True)
            some = total > 0.0
            safe = jnp.where(some, total, 1.0)
            level = jnp.where(some, peaks[j, b] + jnp.log2(safe), VERY_LOW)
            inverse[j, b] = jnp.broadcast_to(1.0 / safe, (rows, head_dim))
            i, local = b // share, b % share
            stats[i] = jnp.where(lane == j * share + local, level, stats[i])

    upper = iota((batch * rows, head_dim), 0) % rows < half

    def gather(j, at, size):
        for pp in range(at // 2, (at + size) // 2):
            both = [
                v_vmem[2 * pp : 2 * pp + 2, 2 * j + g].reshape(2 * page, head_dim)
                for g in range(2)
            ]
            register = pp // 2 % 2
            pltpu.matmul_push_rhs(
                jnp.concatenate(both, axis=1), staging_register=register, mxu_index=pp % 2
            )
            pltpu.matmul_acc_lhs(
                value_acc[2 * j + pp % 2],
                jnp.concatenate([spread[j, 2 * pp], spread[j, 2 * pp + 1]], axis=1),
                load_staged_rhs=register,
            )

    def merge(j):
        found = pltpu.matmul_pop(value_acc[2 * j]) + pltpu.matmul_pop(value_acc[2 * j + 1])
        return jnp.where(upper, found[:, :head_dim], found[:, head_dim:])

    def post(start):
        @pl.when(jnp.logical_not(mine))
        def _():
            for i in range(parts):
                start(i)

        @pl.when(mine)
        def _():
            for i, o in enumerate(owners):
                @pl.when(me != o)
                def _():
                    start(i)

    def post_stats():
        for i in range(parts):
            stat_out[i] = stats[i]
        pl.semaphore_wait(barrier, jnp.where(mine, parts - 1, parts))
        post(lambda i: stat_copy(i).start())
        for i, o in enumerate(owners):
            @pl.when(own(o))
            def _():
                stat_in[slot] = stat_out[i]

    def post_numer(j, numer):
        scale = jnp.concatenate([inverse[j, b] for b in range(batch)], axis=0)
        num_out[j] = (numer * scale).reshape(parts, share * rows, head_dim)
        post(lambda i: num_copy(j, i).start())
        for i, o in enumerate(owners):
            @pl.when(own(o))
            def _():
                num_in[j, slot] = num_out[j, i]

    first = v_copies[0][2]
    for p in range(first):
        soften(0, p)
    owed = None
    for j, at, size, copy in v_copies:
        copy.wait()
        gather(j, at, size)
        if j == 0:
            for p in range(at + size, min(at + size + first, slots)):
                soften(0, p)
            for other in range(1, pairs):
                for p in range(at, at + size):
                    soften(other, p)
            if at + size == slots:
                for other in range(pairs):
                    account(other)
        if owed is not None:
            if owed == 0:
                post_stats()
            post_numer(owed, merge(owed))
        owed = j if at + size == slots else None
    post_numer(owed, merge(owed))

    @pl.when(mine)
    def _():
        columns = {}
        for h in range(sides):
            senders = n - 1 if h == gate else n
            bytes_of(stat_in.at[pl.ds(0, senders)], stat_recv.at[h]).wait_recv()
            levels = stat_in[h * n : (h + 1) * n]
            scales = jnp.exp2(levels - jnp.max(levels, axis=0, keepdims=True))
            scales = scales / jnp.sum(scales, axis=0, keepdims=True)
            for s in range(n):
                for at in range(pairs * share):
                    columns[h, s, at] = jnp.broadcast_to(
                        scales[s][:, at : at + 1], (rows, head_dim)
                    )
        for h in range(sides):
            senders = n - 1 if h == gate else n
            blocks = []
            for j in range(pairs):
                bytes_of(num_in.at[j, pl.ds(0, senders)], num_recv.at[j, h]).wait_recv()
                for local in range(share):
                    blocks.append(
                        sum(
                            columns[h, s, j * share + local]
                            * num_in[j, h * n + s, local * rows : (local + 1) * rows, :]
                            for s in range(n)
                        )
                    )
            for local in range(share):
                whole = [blocks[j * share + local] for j in range(pairs)]
                whole = jnp.concatenate(whole, axis=0).astype(out_ref.dtype)
                done_ref[h, local] = whole
                if h == gate:
                    out_ref[rank * share + local] = whole
            for other, seq in others():
                if other == h:
                    fin_copy(h, seq, rank).start()

    @pl.when(jnp.logical_not(mine))
    def _():
        bytes_of(stat_out, stat_send).wait_send()
        bytes_of(num_out, num_send).wait_send()
        bytes_of(out_ref, fin_recv).wait_recv()

    @pl.when(mine)
    def _():
        if parts > 1:
            bytes_of(stat_out.at[pl.ds(0, parts - 1)], stat_send).wait_send()
            bytes_of(num_out.at[:, pl.ds(0, parts - 1)], num_send).wait_send()
            bytes_of(out_ref.at[pl.ds(0, (parts - 1) * share)], fin_recv).wait_recv()
        bytes_of(tally, fin_send).wait_send()


def scoped(n, sides, table_width, owners, batch, heads, slots, pairs, *refs):
    rows = heads // pairs
    pieces = KEY_PIECES
    accs = []
    for i in range(pieces):
        accs.append(pltpu.ACC(i % 2)((slots * heads // pieces, 256), jnp.float32))
    tiles = slots // 2 * pairs
    for i in range(tiles):
        accs.append(pltpu.ACC(i % 2)((2 * rows, 256), jnp.float32))
    for i in range(2 * pairs):
        accs.append(pltpu.ACC(i % 2)((batch * rows, 256), jnp.float32))

    def body(*accs):
        attend(
            n,
            sides,
            table_width,
            owners,
            accs[:pieces],
            accs[pieces : pieces + tiles],
            accs[pieces + tiles :],
            *refs,
        )

    pl.run_scoped(body, *accs)


def shards(n, sides, owners, query_rows, cache_keys, cache_values, page_table, seq_lengths):
    slots, kv_heads, page, head_dim = cache_keys.shape
    batch, heads, _ = query_rows.shape
    pool = page_table.shape[0]
    rows, pairs = 2 * heads // kv_heads, kv_heads // 2
    parts = len(owners)
    share = batch // parts
    f32, bf16 = jnp.float32, jnp.bfloat16
    hbm = pl.BlockSpec(memory_space=pl.ANY)
    dma = pltpu.SemaphoreType.DMA
    return pl.pallas_call(
        functools.partial(scoped, n, sides, pool // batch, owners, batch, heads, slots, pairs),
        out_shape=pltpu.VMEM((batch, heads, head_dim), bf16),
        in_specs=[hbm] * 5,
        out_specs=pl.BlockSpec(memory_space=pltpu.VMEM),
        scratch_shapes=[
            pltpu.VMEM((batch, heads, head_dim), bf16),
            pltpu.VMEM((pool,), jnp.int32),
            pltpu.SMEM((batch,), jnp.int32),
            pltpu.VMEM((slots, kv_heads, page, head_dim), bf16),
            pltpu.VMEM((slots, kv_heads, page, head_dim), bf16),
            pltpu.VMEM((slots, page), f32),
            pltpu.VMEM((slots, page), f32),
            pltpu.VMEM((2, slots * heads, head_dim), bf16),
            pltpu.VMEM((slots, batch * rows, page), bf16),
            pltpu.VMEM((slots, pairs, rows, page), f32),
            pltpu.VMEM((pairs, slots, batch * rows, page), bf16),
            pltpu.VMEM((slots, batch, page), f32),
            pltpu.VMEM((batch, pairs, rows, page), f32),
            pltpu.VMEM((1, page), jnp.int32),
            pltpu.SMEM((1, page), jnp.int32),
            pltpu.VMEM((sides, share, heads, head_dim), bf16),
            pltpu.VMEM((sides * n - 1, share, heads, head_dim), bf16),
            pltpu.VMEM((parts, rows, page), f32),
            pltpu.VMEM((sides * n, rows, page), f32),
            pltpu.VMEM((pairs, parts, share * rows, head_dim), f32),
            pltpu.VMEM((pairs, sides * n, share * rows, head_dim), f32),
            dma((3,)),
            dma((KEY_PIECES,)),
            dma((EARLY,)),
            dma,
            dma((sides,)),
            dma,
            dma((pairs, sides)),
            dma,
            dma,
        ],
        compiler_params=pltpu.CompilerParams(collective_id=0, has_side_effects=True),
    )(query_rows, cache_keys, cache_values, page_table, seq_lengths)


def owners_of(n):
    return tuple(range(n // 2 - 2, n // 2 + 2))


def solution(mesh):
    n = mesh.shape["seq"]
    owners = owners_of(n)
    in_specs = (
        P("grp", "head", None),
        P(("grp", "seq"), "head", None, None),
        P(("grp", "seq"), "head", None, None),
        P("grp"),
        P("grp"),
    )
    return jax.shard_map(
        functools.partial(shards, n, mesh.shape["head"], owners),
        mesh=mesh,
        in_specs=in_specs,
        out_specs=P("grp", "head", None),
        check_vma=False,
    )
```

```python
import functools
import math

import jax
import jax.numpy as jnp
from jax import lax
from jax.experimental import pallas as pl
from jax.experimental.pallas import tpu as pltpu
from jax.sharding import PartitionSpec as P

MESH = pl.DeviceIdType.MESH
VERY_LOW = -1e30
FLOOR = -1e29
KEY_PIECES = 8
VALUE_PIECES = ((1, 1, 1, 1), (2, 2, 2, 1, 1))
EARLY = 1
STEP = 1
PAUSE = 40


def attend(
    n,
    sides,
    table_width,
    owners,
    pick_acc,
    score_acc,
    value_acc,
    q_hbm,
    k_hbm,
    v_hbm,
    pt_hbm,
    len_hbm,
    out_ref,
    q_raw,
    pt_vmem,
    len_smem,
    k_vmem,
    v_vmem,
    slot_seq,
    slot_live,
    picked,
    choose,
    soft,
    spread,
    bias,
    crest,
    row_vmem,
    row_smem,
    done_ref,
    tally,
    stat_out,
    stat_in,
    num_out,
    num_in,
    small_sem,
    k_sem,
    v_sem,
    stat_send,
    stat_recv,
    num_send,
    num_recv,
    fin_send,
    fin_recv,
):
    me = lax.axis_index("seq")
    side = lax.axis_index("head")
    gate = sides - 1
    batch, heads, head_dim = q_raw.shape
    slots, kv_heads, page, _ = k_vmem.shape
    pairs = kv_heads // 2
    half = heads // kv_heads
    rows = 2 * half
    pool = pt_vmem.shape[0]
    f32, bf16 = jnp.float32, jnp.bfloat16
    factor = math.log2(math.e) / math.sqrt(head_dim)

    small = (
        pltpu.make_async_copy(pt_hbm, pt_vmem, small_sem.at[0]),
        pltpu.make_async_copy(len_hbm, len_smem, small_sem.at[1]),
        pltpu.make_async_copy(q_hbm, q_raw, small_sem.at[2]),
    )
    for copy in small:
        copy.start()
    pl.delay(PAUSE)
    span = slots // KEY_PIECES
    k_copies = [
        pltpu.make_async_copy(
            k_hbm.at[pl.ds(i * span, span)], k_vmem.at[pl.ds(i * span, span)], k_sem.at[i]
        )
        for i in range(KEY_PIECES)
    ]
    v_copies = []
    for j in range(pairs):
        cuts = VALUE_PIECES[min(j, 1)]
        unit, at = slots // sum(cuts), 0
        for size in cuts:
            pages = pl.ds(at, size * unit)
            v_copies.append(
                (
                    j,
                    at,
                    size * unit,
                    pltpu.make_async_copy(
                        v_hbm.at[pages, pl.ds(2 * j, 2)],
                        v_vmem.at[pages, pl.ds(2 * j, 2)],
                        v_sem.at[len(v_copies)]
                        if len(v_copies) < EARLY
                        else k_sem.at[len(v_copies) - EARLY],
                    ),
                )
            )
            at += size * unit
    for copy in k_copies:
        copy.start()
    unstarted = [copy for _, _, _, copy in v_copies]
    for _ in range(EARLY):
        unstarted.pop(0).start()

    serves = [
        (side == gate) & functools.reduce(lambda a, b: a | b, [me == o for o in owners[h]])
        for h in range(sides)
    ]
    mine = serves[gate]
    parts = len(owners[0])
    share = batch // parts
    rank = sum(jnp.where(me == o, i, 0) for h in range(sides) for i, o in enumerate(owners[h]))
    targets = [
        sum(jnp.where(side == h, owners[h][i], 0) for h in range(sides)) for i in range(parts)
    ]
    barrier = pltpu.get_barrier_semaphore()

    def members(h):
        for seq in range(n - 1 if h == gate else n):
            yield jnp.where(me <= seq, seq + 1, seq) if h == gate else seq

    for h in range(sides):
        @pl.when(serves[h])
        def _():
            for seq in members(h):
                pl.semaphore_signal(
                    barrier, inc=1, device_id={"seq": seq, "head": h}, device_id_type=MESH
                )

    def stat_copy(i):
        return pltpu.make_async_remote_copy(
            src_ref=stat_out.at[i],
            dst_ref=stat_in.at[me],
            send_sem=stat_send,
            recv_sem=stat_recv,
            device_id={"seq": targets[i], "head": gate},
            device_id_type=MESH,
        )

    def num_copy(j, i):
        return pltpu.make_async_remote_copy(
            src_ref=num_out.at[j, i],
            dst_ref=num_in.at[j, me],
            send_sem=num_send,
            recv_sem=num_recv.at[j],
            device_id={"seq": targets[i], "head": gate},
            device_id_type=MESH,
        )

    def fin_copy(h, seq):
        return pltpu.make_async_remote_copy(
            src_ref=done_ref,
            dst_ref=out_ref.at[pl.ds(rank * share, share)],
            send_sem=fin_send,
            recv_sem=fin_recv,
            device_id={"seq": seq, "head": h},
            device_id_type=MESH,
        )

    def bytes_of(ref, sem):
        return pltpu.make_async_remote_copy(
            src_ref=ref,
            dst_ref=ref,
            send_sem=sem,
            recv_sem=sem,
            device_id={"seq": targets[0], "head": gate},
            device_id_type=MESH,
        )

    def iota(shape, dim):
        return lax.broadcasted_iota(jnp.int32, shape, dim)

    small[0].wait()
    small[1].wait()
    entry = iota((1, pool), 1)
    live = jnp.zeros((1, pool), jnp.int32)
    owner_seq = jnp.zeros((1, pool), jnp.int32)
    for b in range(batch):
        past = entry >= b * table_width
        left = jnp.clip(len_smem[b] - page * (entry - b * table_width), 0, page)
        live = jnp.where(past, left, live)
        owner_seq = jnp.where(past, b, owner_seq)
    hit = pt_vmem[...].reshape(1, pool) == me * slots + iota((slots, pool), 0)
    seq_col = jnp.sum(jnp.where(hit, owner_seq.astype(f32), 0.0), axis=1, keepdims=True)
    live_col = jnp.sum(jnp.where(hit, live.astype(f32), 0.0), axis=1, keepdims=True)
    seq_wide = jnp.broadcast_to(seq_col, (slots, page))
    slot_seq[...] = seq_wide
    slot_live[...] = jnp.broadcast_to(live_col, (slots, page))
    lane = iota((rows, page), 1)
    lane_f = lane.astype(f32)
    diagonal = iota((slots, page), 0) == iota((slots, page), 1)
    seq_row = jnp.sum(jnp.where(diagonal, seq_wide, 0.0), axis=0, keepdims=True)
    seq_row = jnp.where(iota((1, page), 1) < slots, seq_row, -1.0)
    row_vmem[...] = jnp.clip(seq_row.astype(jnp.int32), 0, batch - 1)
    row_copy = pltpu.make_async_copy(row_vmem, row_smem, small_sem.at[0])
    row_copy.start()
    seq_row = jnp.broadcast_to(seq_row, (rows, page))

    small[2].wait()
    column = iota((heads, 2 * batch * heads), 1)
    line = iota((heads, 2 * batch * heads), 0)
    match = column // (batch * heads) == line % rows // half
    mark = jnp.where((column % heads == line) & match, column % (batch * heads) // heads, -1)
    mark = mark.astype(f32)
    queries = q_raw[...].reshape(batch * heads, head_dim)
    blank = jnp.zeros_like(queries)
    queries = jnp.concatenate(
        [
            jnp.concatenate([queries, blank], axis=1),
            jnp.concatenate([blank, queries], axis=1),
        ],
        axis=0,
    )
    for unit in range(2):
        pltpu.matmul_push_rhs(queries, staging_register=0, mxu_index=unit)
    group = slots // len(pick_acc)
    for i, acc in enumerate(pick_acc):
        pick = []
        for pp in range(i * group // 2, (i + 1) * group // 2):
            for j in range(pairs):
                for p in (2 * pp, 2 * pp + 1):
                    seq = slot_seq[p : p + 1, :]
                    seq = jnp.concatenate([seq, seq], axis=1)
                    pick.append(jnp.where(mark[j * rows : (j + 1) * rows] == seq, 1.0, 0.0))
        pick = jnp.concatenate(pick, axis=0).astype(bf16)
        pltpu.matmul_acc_lhs(acc, pick, load_staged_rhs=0 if i < 2 else None)
    def store_picks(i):
        found = pltpu.matmul_pop(pick_acc[i]).astype(bf16)
        here = pl.ds(i * group * heads, group * heads)
        picked[0, here] = found[:, :head_dim]
        picked[1, here] = found[:, head_dim:]

    store_picks(0)
    wide = (iota((batch * rows, page), 0) // rows).astype(f32)
    each = iota((batch, page), 0).astype(f32)
    peaks = {(j, b): jnp.full((rows, page), VERY_LOW, f32) for j in range(pairs) for b in range(batch)}
    sums = [jnp.zeros((rows, page), f32) for _ in range(pairs)]

    def prepare(p):
        choose[p] = jnp.where(wide == slot_seq[p : p + 1, :], 1.0, 0.0).astype(bf16)
        bias[p] = jnp.where(each == slot_seq[p : p + 1, :], 0.0, VERY_LOW)

    def score(pp, j):
        both = [
            k_vmem[2 * pp : 2 * pp + 2, 2 * j + g].reshape(2 * page, head_dim) for g in range(2)
        ]
        tile = pp * pairs + j
        register = tile // 2 % 2
        pltpu.matmul_push_rhs(
            jnp.concatenate(both, axis=1),
            staging_register=register,
            mxu_index=tile % 2,
            transpose=True,
        )
        pltpu.matmul_acc_lhs(
            score_acc[tile],
            jnp.concatenate([picked[g, pl.ds(tile * 2 * rows, 2 * rows)] for g in range(2)], axis=1),
            load_staged_rhs=register,
        )

    def scores(pp, j):
        found = pltpu.matmul_pop(score_acc[pp * pairs + j])
        return [found[i * rows : (i + 1) * rows, i * page : (i + 1) * page] for i in range(2)]

    def settle(p, j, s):
        s = jnp.where(lane_f < slot_live[p : p + 1, :], s * factor, VERY_LOW)
        soft[p, j] = s
        for b in range(batch):
            peaks[j, b] = jnp.maximum(peaks[j, b], s + bias[p, b : b + 1, :])

    for i in range(KEY_PIECES + 1):
        if i < KEY_PIECES:
            k_copies[i].wait()
            for _ in range(min(STEP, len(unstarted))):
                unstarted.pop(0).start()
            for pp in range(i * span // 2, (i + 1) * span // 2):
                for j in range(pairs):
                    score(pp, j)
            if i + 1 < KEY_PIECES:
                store_picks(i + 1)
            for p in range(i * span, (i + 1) * span):
                prepare(p)
        if i > 0:
            for pp in range((i - 1) * span // 2, i * span // 2):
                for j in range(pairs):
                    for k, found in enumerate(scores(pp, j)):
                        settle(2 * pp + k, j, found)

    row_copy.wait()
    for copy in unstarted:
        copy.start()
    for key in peaks:
        j, b = key
        peaks[key] = jnp.maximum(jnp.max(peaks[key], axis=1, keepdims=True), FLOOR)
        crest[b, j] = jnp.broadcast_to(peaks[key], (rows, page))

    def soften(j, p):
        seq = jnp.clip(row_smem[0, p], 0, batch - 1)
        w = jnp.exp2(soft[p, j] - crest[seq, j])
        sums[j] = jnp.where(lane == p, jnp.sum(w, axis=1, keepdims=True), sums[j])
        w = jnp.concatenate([w] * 2, axis=0).astype(bf16)
        w = jnp.concatenate([w] * (batch // 2), axis=0)
        spread[j, p] = w * choose[p]

    stats = [jnp.zeros((rows, page), f32) for _ in range(parts)]
    inverse = {}

    def account(j):
        for b in range(batch):
            total = jnp.where(seq_row == float(b), sums[j], 0.0)
            total = jnp.sum(total, axis=1, keepdims=True)
            some = total > 0.0
            safe = jnp.where(some, total, 1.0)
            level = jnp.where(some, peaks[j, b] + jnp.log2(safe), VERY_LOW)
            inverse[j, b] = jnp.broadcast_to(1.0 / safe, (rows, head_dim))
            i, local = b // share, b % share
            stats[i] = jnp.where(lane == j * share + local, level, stats[i])

    upper = iota((batch * rows, head_dim), 0) % rows < half

    def gather(j, at, size):
        for pp in range(at // 2, (at + size) // 2):
            both = [
                v_vmem[2 * pp : 2 * pp + 2, 2 * j + g].reshape(2 * page, head_dim)
                for g in range(2)
            ]
            register = pp // 2 % 2
            pltpu.matmul_push_rhs(
                jnp.concatenate(both, axis=1), staging_register=register, mxu_index=pp % 2
            )
            pltpu.matmul_acc_lhs(
                value_acc[2 * j + pp % 2],
                jnp.concatenate([spread[j, 2 * pp], spread[j, 2 * pp + 1]], axis=1),
                load_staged_rhs=register,
            )

    def merge(j):
        found = pltpu.matmul_pop(value_acc[2 * j]) + pltpu.matmul_pop(value_acc[2 * j + 1])
        return jnp.where(upper, found[:, :head_dim], found[:, head_dim:])

    def post(start, keep):
        @pl.when(jnp.logical_not(mine))
        def _():
            for i in range(parts):
                start(i)

        @pl.when(mine)
        def _():
            for i, o in enumerate(owners[gate]):
                @pl.when(me != o)
                def _():
                    start(i)

                @pl.when(me == o)
                def _():
                    keep(i)

    def post_stats():
        for i in range(parts):
            stat_out[i] = stats[i]
        pl.semaphore_wait(barrier, jnp.where(mine, parts - 1, parts))

        def keep(i):
            stat_in[me] = stat_out[i]

        post(lambda i: stat_copy(i).start(), keep)

    def post_numer(j, numer):
        scale = jnp.concatenate([inverse[j, b] for b in range(batch)], axis=0)
        num_out[j] = (numer * scale).reshape(parts, share * rows, head_dim)

        def keep(i):
            num_in[j, me] = num_out[j, i]

        post(lambda i: num_copy(j, i).start(), keep)

    first = v_copies[0][2]
    for p in range(first):
        soften(0, p)
    owed = None
    for j, at, size, copy in v_copies:
        copy.wait()
        gather(j, at, size)
        if j == 0:
            for p in range(at + size, min(at + size + first, slots)):
                soften(0, p)
            for other in range(1, pairs):
                for p in range(at, at + size):
                    soften(other, p)
            if at + size == slots:
                for other in range(pairs):
                    account(other)
        if owed is not None:
            if owed == 0:
                post_stats()
            post_numer(owed, merge(owed))
        owed = j if at + size == slots else None
    post_numer(owed, merge(owed))

    def combine(h):
        senders = n - 1 if h == gate else n
        bytes_of(stat_in.at[pl.ds(0, senders)], stat_recv).wait_recv()
        levels = stat_in[...]
        scales = jnp.exp2(levels - jnp.max(levels, axis=0, keepdims=True))
        scales = scales / jnp.sum(scales, axis=0, keepdims=True)
        columns = {}
        for s in range(n):
            for at in range(pairs * share):
                columns[s, at] = jnp.broadcast_to(scales[s][:, at : at + 1], (rows, head_dim))
        blocks = []
        for j in range(pairs):
            bytes_of(num_in.at[j, pl.ds(0, senders)], num_recv.at[j]).wait_recv()
            for local in range(share):
                here = pl.ds(local * rows, rows)
                blocks.append(
                    sum(columns[s, j * share + local] * num_in[j, s, here, :] for s in range(n))
                )
        for local in range(share):
            whole = [blocks[j * share + local] for j in range(pairs)]
            whole = jnp.concatenate(whole, axis=0).astype(out_ref.dtype)
            done_ref[local] = whole
            if h == gate:
                out_ref[rank * share + local] = whole
        for seq in members(h):
            fin_copy(h, seq).start()

    for h in range(sides):
        @pl.when(serves[h])
        def _():
            combine(h)

    @pl.when(jnp.logical_not(mine))
    def _():
        bytes_of(stat_out, stat_send).wait_send()
        bytes_of(num_out, num_send).wait_send()
        bytes_of(out_ref, fin_recv).wait_recv()

    @pl.when(mine)
    def _():
        if parts > 1:
            bytes_of(stat_out.at[pl.ds(0, parts - 1)], stat_send).wait_send()
            bytes_of(num_out.at[:, pl.ds(0, parts - 1)], num_send).wait_send()
            bytes_of(out_ref.at[pl.ds(0, (parts - 1) * share)], fin_recv).wait_recv()

    for h in range(sides):
        @pl.when(serves[h])
        def _():
            bytes_of(tally.at[pl.ds(0, n - 1 if h == gate else n)], fin_send).wait_send()


def scoped(n, sides, table_width, owners, batch, heads, slots, pairs, *refs):
    rows = heads // pairs
    pieces = KEY_PIECES
    accs = []
    for i in range(pieces):
        accs.append(pltpu.ACC(i % 2)((slots * heads // pieces, 256), jnp.float32))
    tiles = slots // 2 * pairs
    for i in range(tiles):
        accs.append(pltpu.ACC(i % 2)((2 * rows, 256), jnp.float32))
    for i in range(2 * pairs):
        accs.append(pltpu.ACC(i % 2)((batch * rows, 256), jnp.float32))

    def body(*accs):
        attend(
            n,
            sides,
            table_width,
            owners,
            accs[:pieces],
            accs[pieces : pieces + tiles],
            accs[pieces + tiles :],
            *refs,
        )

    pl.run_scoped(body, *accs)


def shards(n, sides, owners, query_rows, cache_keys, cache_values, page_table, seq_lengths):
    slots, kv_heads, page, head_dim = cache_keys.shape
    batch, heads, _ = query_rows.shape
    pool = page_table.shape[0]
    rows, pairs = 2 * heads // kv_heads, kv_heads // 2
    parts = len(owners[0])
    share = batch // parts
    f32, bf16 = jnp.float32, jnp.bfloat16
    hbm = pl.BlockSpec(memory_space=pl.ANY)
    dma = pltpu.SemaphoreType.DMA
    return pl.pallas_call(
        functools.partial(scoped, n, sides, pool // batch, owners, batch, heads, slots, pairs),
        out_shape=pltpu.VMEM((batch, heads, head_dim), bf16),
        in_specs=[hbm] * 5,
        out_specs=pl.BlockSpec(memory_space=pltpu.VMEM),
        scratch_shapes=[
            pltpu.VMEM((batch, heads, head_dim), bf16),
            pltpu.VMEM((pool,), jnp.int32),
            pltpu.SMEM((batch,), jnp.int32),
            pltpu.VMEM((slots, kv_heads, page, head_dim), bf16),
            pltpu.VMEM((slots, kv_heads, page, head_dim), bf16),
            pltpu.VMEM((slots, page), f32),
            pltpu.VMEM((slots, page), f32),
            pltpu.VMEM((2, slots * heads, head_dim), bf16),
            pltpu.VMEM((slots, batch * rows, page), bf16),
            pltpu.VMEM((slots, pairs, rows, page), f32),
            pltpu.VMEM((pairs, slots, batch * rows, page), bf16),
            pltpu.VMEM((slots, batch, page), f32),
            pltpu.VMEM((batch, pairs, rows, page), f32),
            pltpu.VMEM((1, page), jnp.int32),
            pltpu.SMEM((1, page), jnp.int32),
            pltpu.VMEM((share, heads, head_dim), bf16),
            pltpu.VMEM((n, share, heads, head_dim), bf16),
            pltpu.VMEM((parts, rows, page), f32),
            pltpu.VMEM((n, rows, page), f32),
            pltpu.VMEM((pairs, parts, share * rows, head_dim), f32),
            pltpu.VMEM((pairs, n, share * rows, head_dim), f32),
            dma((3,)),
            dma((KEY_PIECES,)),
            dma((EARLY,)),
            dma,
            dma,
            dma,
            dma((pairs,)),
            dma,
            dma,
        ],
        compiler_params=pltpu.CompilerParams(collective_id=0, has_side_effects=True),
    )(query_rows, cache_keys, cache_values, page_table, seq_lengths)


def owners_of(n, sides):
    even = tuple(range(0, n, n // 4))
    return tuple(tuple(o + h for o in even) for h in range(sides))


def solution(mesh):
    n = mesh.shape["seq"]
    owners = owners_of(n, mesh.shape["head"])
    in_specs = (
        P("grp", "head", None),
        P(("grp", "seq"), "head", None, None),
        P(("grp", "seq"), "head", None, None),
        P("grp"),
        P("grp"),
    )
    return jax.shard_map(
        functools.partial(shards, n, mesh.shape["head"], owners),
        mesh=mesh,
        in_specs=in_specs,
        out_specs=P("grp", "head", None),
        check_vma=False,
    )
```

```python
import functools
import math

import jax
import jax.numpy as jnp
from jax import lax
from jax.experimental import pallas as pl
from jax.experimental.pallas import tpu as pltpu
from jax.sharding import PartitionSpec as P

MESH = pl.DeviceIdType.MESH
VERY_LOW = -1e30
FLOOR = -1e29
KEY_PIECES = 8
VALUE_PIECES = ((1, 1, 1, 1), (2, 2, 2, 1, 1))
EARLY = 1
STEP = 1
PAUSE = 40


def attend(
    n,
    sides,
    table_width,
    owners,
    pick_acc,
    score_acc,
    value_acc,
    q_hbm,
    k_hbm,
    v_hbm,
    pt_hbm,
    len_hbm,
    out_ref,
    q_raw,
    pt_vmem,
    len_smem,
    k_vmem,
    v_vmem,
    slot_seq,
    slot_live,
    picked,
    choose,
    soft,
    spread,
    bias,
    crest,
    row_vmem,
    row_smem,
    done_ref,
    tally,
    rest_scale,
    rest,
    scale_in,
    rest_in,
    far_in,
    stat_out,
    stat_in,
    num_out,
    num_in,
    small_sem,
    k_sem,
    v_sem,
    stat_send,
    stat_recv,
    num_send,
    num_recv,
    fin_send,
    fin_recv,
    far_send,
    far_recv,
    scale_send,
    scale_recv,
    rest_send,
    rest_recv,
):
    me = lax.axis_index("seq")
    side = lax.axis_index("head")
    gate = sides - 1
    batch, heads, head_dim = q_raw.shape
    slots, kv_heads, page, _ = k_vmem.shape
    pairs = kv_heads // 2
    half = heads // kv_heads
    rows = 2 * half
    pool = pt_vmem.shape[0]
    f32, bf16 = jnp.float32, jnp.bfloat16
    factor = math.log2(math.e) / math.sqrt(head_dim)

    small = (
        pltpu.make_async_copy(pt_hbm, pt_vmem, small_sem.at[0]),
        pltpu.make_async_copy(len_hbm, len_smem, small_sem.at[1]),
        pltpu.make_async_copy(q_hbm, q_raw, small_sem.at[2]),
    )
    for copy in small:
        copy.start()
    pl.delay(PAUSE)
    span = slots // KEY_PIECES
    k_copies = [
        pltpu.make_async_copy(
            k_hbm.at[pl.ds(i * span, span)], k_vmem.at[pl.ds(i * span, span)], k_sem.at[i]
        )
        for i in range(KEY_PIECES)
    ]
    v_copies = []
    for j in range(pairs):
        cuts = VALUE_PIECES[min(j, 1)]
        unit, at = slots // sum(cuts), 0
        for size in cuts:
            pages = pl.ds(at, size * unit)
            v_copies.append(
                (
                    j,
                    at,
                    size * unit,
                    pltpu.make_async_copy(
                        v_hbm.at[pages, pl.ds(2 * j, 2)],
                        v_vmem.at[pages, pl.ds(2 * j, 2)],
                        v_sem.at[len(v_copies)]
                        if len(v_copies) < EARLY
                        else k_sem.at[len(v_copies) - EARLY],
                    ),
                )
            )
            at += size * unit
    for copy in k_copies:
        copy.start()
    unstarted = [copy for _, _, _, copy in v_copies]
    for _ in range(EARLY):
        unstarted.pop(0).start()

    serves = [
        (side == gate) & functools.reduce(lambda a, b: a | b, [me == o for o in owners[h]])
        for h in range(sides)
    ]
    mine = serves[gate]
    parts = len(owners[0])
    share = batch // parts
    rank = sum(jnp.where(me == o, i, 0) for h in range(sides) for i, o in enumerate(owners[h]))
    targets = [
        sum(jnp.where(side == h, owners[h][i], 0) for h in range(sides)) for i in range(parts)
    ]
    near, far = 0, n - 1
    is_near = (side != gate) & (me == near)
    is_far = (side != gate) & (me == far)
    late = jnp.where(is_far, 1, 0)
    barrier = pltpu.get_barrier_semaphore()

    @pl.when(is_near)
    def _():
        pl.semaphore_signal(barrier, inc=1, device_id={"seq": far}, device_id_type=MESH)

    def members(h):
        for seq in range(n - 1 if h == gate else n):
            yield jnp.where(me <= seq, seq + 1, seq) if h == gate else seq

    for h in range(sides):
        @pl.when(serves[h])
        def _():
            for seq in members(h):
                pl.semaphore_signal(
                    barrier, inc=1, device_id={"seq": seq, "head": h}, device_id_type=MESH
                )

    def stat_copy(i):
        return pltpu.make_async_remote_copy(
            src_ref=stat_out.at[i],
            dst_ref=stat_in.at[me],
            send_sem=stat_send,
            recv_sem=stat_recv,
            device_id={"seq": targets[i], "head": gate},
            device_id_type=MESH,
        )

    def num_copy(j, i):
        return pltpu.make_async_remote_copy(
            src_ref=num_out.at[j, i],
            dst_ref=num_in.at[j, me],
            send_sem=num_send,
            recv_sem=num_recv.at[j, late],
            device_id={"seq": targets[i], "head": gate},
            device_id_type=MESH,
        )

    def near_copy(src, dst, send, recv):
        return pltpu.make_async_remote_copy(
            src_ref=src,
            dst_ref=dst,
            send_sem=send,
            recv_sem=recv,
            device_id={"seq": near, "head": 0},
            device_id_type=MESH,
        )

    def fin_copy(h, seq):
        return pltpu.make_async_remote_copy(
            src_ref=done_ref,
            dst_ref=out_ref.at[pl.ds(rank * share, share)],
            send_sem=fin_send,
            recv_sem=fin_recv,
            device_id={"seq": seq, "head": h},
            device_id_type=MESH,
        )

    def bytes_of(ref, sem):
        return pltpu.make_async_remote_copy(
            src_ref=ref,
            dst_ref=ref,
            send_sem=sem,
            recv_sem=sem,
            device_id={"seq": targets[0], "head": gate},
            device_id_type=MESH,
        )

    def iota(shape, dim):
        return lax.broadcasted_iota(jnp.int32, shape, dim)

    small[0].wait()
    small[1].wait()
    entry = iota((1, pool), 1)
    live = jnp.zeros((1, pool), jnp.int32)
    owner_seq = jnp.zeros((1, pool), jnp.int32)
    for b in range(batch):
        past = entry >= b * table_width
        left = jnp.clip(len_smem[b] - page * (entry - b * table_width), 0, page)
        live = jnp.where(past, left, live)
        owner_seq = jnp.where(past, b, owner_seq)
    hit = pt_vmem[...].reshape(1, pool) == me * slots + iota((slots, pool), 0)
    seq_col = jnp.sum(jnp.where(hit, owner_seq.astype(f32), 0.0), axis=1, keepdims=True)
    live_col = jnp.sum(jnp.where(hit, live.astype(f32), 0.0), axis=1, keepdims=True)
    seq_wide = jnp.broadcast_to(seq_col, (slots, page))
    slot_seq[...] = seq_wide
    slot_live[...] = jnp.broadcast_to(live_col, (slots, page))
    lane = iota((rows, page), 1)
    lane_f = lane.astype(f32)
    diagonal = iota((slots, page), 0) == iota((slots, page), 1)
    seq_row = jnp.sum(jnp.where(diagonal, seq_wide, 0.0), axis=0, keepdims=True)
    seq_row = jnp.where(iota((1, page), 1) < slots, seq_row, -1.0)
    row_vmem[...] = jnp.clip(seq_row.astype(jnp.int32), 0, batch - 1)
    row_copy = pltpu.make_async_copy(row_vmem, row_smem, small_sem.at[0])
    row_copy.start()
    seq_row = jnp.broadcast_to(seq_row, (rows, page))

    small[2].wait()
    column = iota((heads, 2 * batch * heads), 1)
    line = iota((heads, 2 * batch * heads), 0)
    match = column // (batch * heads) == line % rows // half
    mark = jnp.where((column % heads == line) & match, column % (batch * heads) // heads, -1)
    mark = mark.astype(f32)
    queries = q_raw[...].reshape(batch * heads, head_dim)
    blank = jnp.zeros_like(queries)
    queries = jnp.concatenate(
        [
            jnp.concatenate([queries, blank], axis=1),
            jnp.concatenate([blank, queries], axis=1),
        ],
        axis=0,
    )
    for unit in range(2):
        pltpu.matmul_push_rhs(queries, staging_register=0, mxu_index=unit)
    group = slots // len(pick_acc)
    for i, acc in enumerate(pick_acc):
        pick = []
        for pp in range(i * group // 2, (i + 1) * group // 2):
            for j in range(pairs):
                for p in (2 * pp, 2 * pp + 1):
                    seq = slot_seq[p : p + 1, :]
                    seq = jnp.concatenate([seq, seq], axis=1)
                    pick.append(jnp.where(mark[j * rows : (j + 1) * rows] == seq, 1.0, 0.0))
        pick = jnp.concatenate(pick, axis=0).astype(bf16)
        pltpu.matmul_acc_lhs(acc, pick, load_staged_rhs=0 if i < 2 else None)
    def store_picks(i):
        found = pltpu.matmul_pop(pick_acc[i]).astype(bf16)
        here = pl.ds(i * group * heads, group * heads)
        picked[0, here] = found[:, :head_dim]
        picked[1, here] = found[:, head_dim:]

    store_picks(0)
    wide = (iota((batch * rows, page), 0) // rows).astype(f32)
    each = iota((batch, page), 0).astype(f32)
    peaks = {(j, b): jnp.full((rows, page), VERY_LOW, f32) for j in range(pairs) for b in range(batch)}
    sums = [jnp.zeros((rows, page), f32) for _ in range(pairs)]

    def prepare(p):
        choose[p] = jnp.where(wide == slot_seq[p : p + 1, :], 1.0, 0.0).astype(bf16)
        bias[p] = jnp.where(each == slot_seq[p : p + 1, :], 0.0, VERY_LOW)

    def score(pp, j):
        both = [
            k_vmem[2 * pp : 2 * pp + 2, 2 * j + g].reshape(2 * page, head_dim) for g in range(2)
        ]
        tile = pp * pairs + j
        register = tile // 2 % 2
        pltpu.matmul_push_rhs(
            jnp.concatenate(both, axis=1),
            staging_register=register,
            mxu_index=tile % 2,
            transpose=True,
        )
        pltpu.matmul_acc_lhs(
            score_acc[tile],
            jnp.concatenate([picked[g, pl.ds(tile * 2 * rows, 2 * rows)] for g in range(2)], axis=1),
            load_staged_rhs=register,
        )

    def scores(pp, j):
        found = pltpu.matmul_pop(score_acc[pp * pairs + j])
        return [found[i * rows : (i + 1) * rows, i * page : (i + 1) * page] for i in range(2)]

    def settle(p, j, s):
        s = jnp.where(lane_f < slot_live[p : p + 1, :], s * factor, VERY_LOW)
        soft[p, j] = s
        for b in range(batch):
            peaks[j, b] = jnp.maximum(peaks[j, b], s + bias[p, b : b + 1, :])

    for i in range(KEY_PIECES + 1):
        if i < KEY_PIECES:
            k_copies[i].wait()
            for _ in range(min(STEP, len(unstarted))):
                unstarted.pop(0).start()
            for pp in range(i * span // 2, (i + 1) * span // 2):
                for j in range(pairs):
                    score(pp, j)
            if i + 1 < KEY_PIECES:
                store_picks(i + 1)
            for p in range(i * span, (i + 1) * span):
                prepare(p)
        if i > 0:
            for pp in range((i - 1) * span // 2, i * span // 2):
                for j in range(pairs):
                    for k, found in enumerate(scores(pp, j)):
                        settle(2 * pp + k, j, found)

    row_copy.wait()
    for copy in unstarted:
        copy.start()
    for key in peaks:
        j, b = key
        peaks[key] = jnp.maximum(jnp.max(peaks[key], axis=1, keepdims=True), FLOOR)
        crest[b, j] = jnp.broadcast_to(peaks[key], (rows, page))

    def soften(j, p):
        seq = jnp.clip(row_smem[0, p], 0, batch - 1)
        w = jnp.exp2(soft[p, j] - crest[seq, j])
        sums[j] = jnp.where(lane == p, jnp.sum(w, axis=1, keepdims=True), sums[j])
        w = jnp.concatenate([w] * 2, axis=0).astype(bf16)
        w = jnp.concatenate([w] * (batch // 2), axis=0)
        spread[j, p] = w * choose[p]

    stats = [jnp.zeros((rows, page), f32) for _ in range(parts)]
    inverse = {}

    def account(j):
        for b in range(batch):
            total = jnp.where(seq_row == float(b), sums[j], 0.0)
            total = jnp.sum(total, axis=1, keepdims=True)
            some = total > 0.0
            safe = jnp.where(some, total, 1.0)
            level = jnp.where(some, peaks[j, b] + jnp.log2(safe), VERY_LOW)
            inverse[j, b] = jnp.broadcast_to(1.0 / safe, (rows, head_dim))
            i, local = b // share, b % share
            stats[i] = jnp.where(lane == j * share + local, level, stats[i])

    upper = iota((batch * rows, head_dim), 0) % rows < half

    def gather(j, at, size):
        for pp in range(at // 2, (at + size) // 2):
            both = [
                v_vmem[2 * pp : 2 * pp + 2, 2 * j + g].reshape(2 * page, head_dim)
                for g in range(2)
            ]
            register = pp // 2 % 2
            pltpu.matmul_push_rhs(
                jnp.concatenate(both, axis=1), staging_register=register, mxu_index=pp % 2
            )
            pltpu.matmul_acc_lhs(
                value_acc[2 * j + pp % 2],
                jnp.concatenate([spread[j, 2 * pp], spread[j, 2 * pp + 1]], axis=1),
                load_staged_rhs=register,
            )

    def merge(j):
        found = pltpu.matmul_pop(value_acc[2 * j]) + pltpu.matmul_pop(value_acc[2 * j + 1])
        return jnp.where(upper, found[:, :head_dim], found[:, head_dim:])

    def post(start, keep):
        @pl.when(jnp.logical_not(mine))
        def _():
            for i in range(parts):
                start(i)

        @pl.when(mine)
        def _():
            for i, o in enumerate(owners[gate]):
                @pl.when(me != o)
                def _():
                    start(i)

                @pl.when(me == o)
                def _():
                    keep(i)

    def post_stats():
        for i in range(parts):
            stat_out[i] = stats[i]
        pl.semaphore_wait(barrier, jnp.where(mine, parts - 1, parts) + late)

        def keep(i):
            stat_in[me] = stat_out[i]

        post(lambda i: stat_copy(i).start(), keep)

    def post_numer(j, numer):
        scale = jnp.concatenate([inverse[j, b] for b in range(batch)], axis=0)
        num_out[j] = (numer * scale).reshape(parts, share * rows, head_dim)

        def keep(i):
            num_in[j, me] = num_out[j, i]

        @pl.when(is_far)
        def _():
            near_copy(num_out.at[j], far_in.at[j], far_send, far_recv).start()

        post(lambda i: num_copy(j, i).start(), keep)

    first = v_copies[0][2]
    for p in range(first):
        soften(0, p)
    owed = None
    for j, at, size, copy in v_copies:
        copy.wait()
        gather(j, at, size)
        if j == 0:
            for p in range(at + size, min(at + size + first, slots)):
                soften(0, p)
            for other in range(1, pairs):
                for p in range(at, at + size):
                    soften(other, p)
            if at + size == slots:
                for other in range(pairs):
                    account(other)
        if owed is not None:
            if owed == 0:
                post_stats()
            post_numer(owed, merge(owed))
        owed = j if at + size == slots else None
    post_numer(owed, merge(owed))

    def combine(h):
        senders = n - 1 if h == gate else n
        bytes_of(stat_in.at[pl.ds(0, senders)], stat_recv).wait_recv()
        levels = stat_in[...]
        scales = jnp.exp2(levels - jnp.max(levels, axis=0, keepdims=True))
        scales = scales / jnp.sum(scales, axis=0, keepdims=True)
        columns = {}
        for s in range(n):
            for at in range(pairs * share):
                columns[s, at] = jnp.broadcast_to(scales[s][:, at : at + 1], (rows, head_dim))
        if h != gate:
            rest_scale[...] = scales[far]
            near_copy(rest_scale, scale_in.at[rank], scale_send, scale_recv).start()

        def term(s, j, local):
            here = pl.ds(local * rows, rows)
            return columns[s, j * share + local] * num_in[j, s, here, :]

        blocks = {}
        for j in range(pairs):
            bytes_of(num_in.at[j, pl.ds(0, n - 1)], num_recv.at[j, 0]).wait_recv()
            for local in range(share):
                blocks[j, local] = sum(
                    term(s, j, local) for s in range(n) if h == gate or s != far
                )
            if h != gate:
                for local in range(share):
                    rest[j, pl.ds(local * rows, rows), :] = blocks[j, local]
                near_copy(rest.at[j], rest_in.at[j, rank], rest_send, rest_recv).start()
        if h != gate:
            for j in range(pairs):
                bytes_of(num_in.at[j, pl.ds(0, 1)], num_recv.at[j, 1]).wait_recv()
                for local in range(share):
                    blocks[j, local] = blocks[j, local] + term(far, j, local)
        for local in range(share):
            whole = [blocks[j, local] for j in range(pairs)]
            whole = jnp.concatenate(whole, axis=0).astype(out_ref.dtype)
            done_ref[local] = whole
            if h == gate:
                out_ref[rank * share + local] = whole
        for seq in members(h) if h == gate else range(1, n):
            fin_copy(h, seq).start()

    for h in range(sides):
        @pl.when(serves[h])
        def _():
            combine(h)

    @pl.when(jnp.logical_not(mine))
    def _():
        bytes_of(stat_out, stat_send).wait_send()
        bytes_of(num_out, num_send).wait_send()

    @pl.when(is_far)
    def _():
        bytes_of(num_out, far_send).wait_send()

    @pl.when(jnp.logical_not(mine | is_near))
    def _():
        bytes_of(out_ref, fin_recv).wait_recv()

    @pl.when(is_near)
    def _():
        bytes_of(scale_in, scale_recv).wait_recv()
        columns = {}
        for i in range(parts):
            for at in range(pairs * share):
                columns[i, at] = jnp.broadcast_to(
                    scale_in[i][:, at : at + 1], (rows, head_dim)
                )
        bytes_of(rest_in, rest_recv).wait_recv()
        bytes_of(far_in, far_recv).wait_recv()
        for i in range(parts):
            for local in range(share):
                here = pl.ds(local * rows, rows)
                whole = [
                    rest_in[j, i, here, :] + columns[i, j * share + local] * far_in[j, i, here, :]
                    for j in range(pairs)
                ]
                whole = jnp.concatenate(whole, axis=0).astype(out_ref.dtype)
                out_ref[i * share + local] = whole

    @pl.when(mine)
    def _():
        if parts > 1:
            bytes_of(stat_out.at[pl.ds(0, parts - 1)], stat_send).wait_send()
            bytes_of(num_out.at[:, pl.ds(0, parts - 1)], num_send).wait_send()
            bytes_of(out_ref.at[pl.ds(0, (parts - 1) * share)], fin_recv).wait_recv()

    for h in range(sides):
        @pl.when(serves[h])
        def _():
            bytes_of(tally, fin_send).wait_send()
            if h != gate:
                bytes_of(rest_scale, scale_send).wait_send()
                bytes_of(rest, rest_send).wait_send()


def scoped(n, sides, table_width, owners, batch, heads, slots, pairs, *refs):
    rows = heads // pairs
    pieces = KEY_PIECES
    accs = []
    for i in range(pieces):
        accs.append(pltpu.ACC(i % 2)((slots * heads // pieces, 256), jnp.float32))
    tiles = slots // 2 * pairs
    for i in range(tiles):
        accs.append(pltpu.ACC(i % 2)((2 * rows, 256), jnp.float32))
    for i in range(2 * pairs):
        accs.append(pltpu.ACC(i % 2)((batch * rows, 256), jnp.float32))

    def body(*accs):
        attend(
            n,
            sides,
            table_width,
            owners,
            accs[:pieces],
            accs[pieces : pieces + tiles],
            accs[pieces + tiles :],
            *refs,
        )

    pl.run_scoped(body, *accs)


def shards(n, sides, owners, query_rows, cache_keys, cache_values, page_table, seq_lengths):
    slots, kv_heads, page, head_dim = cache_keys.shape
    batch, heads, _ = query_rows.shape
    pool = page_table.shape[0]
    rows, pairs = 2 * heads // kv_heads, kv_heads // 2
    parts = len(owners[0])
    share = batch // parts
    f32, bf16 = jnp.float32, jnp.bfloat16
    hbm = pl.BlockSpec(memory_space=pl.ANY)
    dma = pltpu.SemaphoreType.DMA
    return pl.pallas_call(
        functools.partial(scoped, n, sides, pool // batch, owners, batch, heads, slots, pairs),
        out_shape=pltpu.VMEM((batch, heads, head_dim), bf16),
        in_specs=[hbm] * 5,
        out_specs=pl.BlockSpec(memory_space=pltpu.VMEM),
        scratch_shapes=[
            pltpu.VMEM((batch, heads, head_dim), bf16),
            pltpu.VMEM((pool,), jnp.int32),
            pltpu.SMEM((batch,), jnp.int32),
            pltpu.VMEM((slots, kv_heads, page, head_dim), bf16),
            pltpu.VMEM((slots, kv_heads, page, head_dim), bf16),
            pltpu.VMEM((slots, page), f32),
            pltpu.VMEM((slots, page), f32),
            pltpu.VMEM((2, slots * heads, head_dim), bf16),
            pltpu.VMEM((slots, batch * rows, page), bf16),
            pltpu.VMEM((slots, pairs, rows, page), f32),
            pltpu.VMEM((pairs, slots, batch * rows, page), bf16),
            pltpu.VMEM((slots, batch, page), f32),
            pltpu.VMEM((batch, pairs, rows, page), f32),
            pltpu.VMEM((1, page), jnp.int32),
            pltpu.SMEM((1, page), jnp.int32),
            pltpu.VMEM((share, heads, head_dim), bf16),
            pltpu.VMEM((n - 1, share, heads, head_dim), bf16),
            pltpu.VMEM((rows, page), f32),
            pltpu.VMEM((pairs, share * rows, head_dim), f32),
            pltpu.VMEM((parts, rows, page), f32),
            pltpu.VMEM((pairs, parts, share * rows, head_dim), f32),
            pltpu.VMEM((pairs, parts, share * rows, head_dim), f32),
            pltpu.VMEM((parts, rows, page), f32),
            pltpu.VMEM((n, rows, page), f32),
            pltpu.VMEM((pairs, parts, share * rows, head_dim), f32),
            pltpu.VMEM((pairs, n, share * rows, head_dim), f32),
            dma((3,)),
            dma((KEY_PIECES,)),
            dma((EARLY,)),
            dma,
            dma,
            dma,
            dma((pairs, 2)),
            dma,
            dma,
            dma,
            dma,
            dma,
            dma,
            dma,
            dma,
        ],
        compiler_params=pltpu.CompilerParams(collective_id=0, has_side_effects=True),
    )(query_rows, cache_keys, cache_values, page_table, seq_lengths)


def owners_of(n, sides):
    even = tuple(range(0, n, n // 4))
    return tuple(tuple(o + h for o in even) for h in range(sides))


def solution(mesh):
    n = mesh.shape["seq"]
    owners = owners_of(n, mesh.shape["head"])
    in_specs = (
        P("grp", "head", None),
        P(("grp", "seq"), "head", None, None),
        P(("grp", "seq"), "head", None, None),
        P("grp"),
        P("grp"),
    )
    return jax.shard_map(
        functools.partial(shards, n, mesh.shape["head"], owners),
        mesh=mesh,
        in_specs=in_specs,
        out_specs=P("grp", "head", None),
        check_vma=False,
    )
```

```python
import functools
import math

import jax
import jax.numpy as jnp
from jax import lax
from jax.experimental import pallas as pl
from jax.experimental.pallas import tpu as pltpu
from jax.sharding import PartitionSpec as P

MESH = pl.DeviceIdType.MESH
VERY_LOW = -1e30
FLOOR = -1e29
KEY_PIECES = 8
VALUE_PIECES = ((1, 1, 1, 1), (2, 2, 2, 1, 1))
WINDOW = 8
PAUSE = 20


def attend(
    n,
    sides,
    table_width,
    owners,
    pick_acc,
    score_acc,
    value_acc,
    q_hbm,
    k_hbm,
    v_hbm,
    pt_hbm,
    len_hbm,
    out_ref,
    q_raw,
    pt_vmem,
    len_smem,
    k_vmem,
    v_vmem,
    slot_seq,
    slot_live,
    picked,
    choose,
    soft,
    spread,
    bias,
    crest,
    row_vmem,
    row_smem,
    done_ref,
    tally,
    rest_scale,
    rest,
    scale_in,
    rest_in,
    far_in,
    stat_out,
    stat_in,
    num_out,
    num_in,
    small_sem,
    k_sem,
    stat_send,
    stat_recv,
    num_send,
    num_recv,
    fin_send,
    fin_recv,
    far_send,
    far_recv,
    scale_send,
    scale_recv,
    rest_send,
    rest_recv,
):
    me = lax.axis_index("seq")
    side = lax.axis_index("head")
    gate = sides - 1
    batch, heads, head_dim = q_raw.shape
    slots, kv_heads, page, _ = k_vmem.shape
    pairs = kv_heads // 2
    half = heads // kv_heads
    rows = 2 * half
    pool = pt_vmem.shape[0]
    f32, bf16 = jnp.float32, jnp.bfloat16
    factor = math.log2(math.e) / math.sqrt(head_dim)

    small = (
        pltpu.make_async_copy(pt_hbm, pt_vmem, small_sem.at[0]),
        pltpu.make_async_copy(len_hbm, len_smem, small_sem.at[1]),
        pltpu.make_async_copy(q_hbm, q_raw, small_sem.at[2]),
    )
    for copy in small:
        copy.start()
    serves = [
        (side == gate) & functools.reduce(lambda a, b: a | b, [me == o for o in owners[h]])
        for h in range(sides)
    ]
    mine = serves[gate]
    parts = len(owners[0])
    share = batch // parts
    rank = sum(jnp.where(me == o, i, 0) for h in range(sides) for i, o in enumerate(owners[h]))
    targets = [
        sum(jnp.where(side == h, owners[h][i], 0) for h in range(sides)) for i in range(parts)
    ]
    near, far = 0, n - 1
    is_near = (side != gate) & (me == near)
    is_far = (side != gate) & (me == far)
    late = jnp.where(is_far, 1, 0)
    barrier = pltpu.get_barrier_semaphore()

    def members(h):
        for seq in range(n - 1 if h == gate else n):
            yield jnp.where(me <= seq, seq + 1, seq) if h == gate else seq

    for h in range(sides):
        @pl.when(serves[h])
        def _():
            for seq in members(h):
                pl.semaphore_signal(
                    barrier, inc=1, device_id={"seq": seq, "head": h}, device_id_type=MESH
                )

    @pl.when(is_near)
    def _():
        pl.semaphore_signal(barrier, inc=1, device_id={"seq": far}, device_id_type=MESH)

    pl.delay(PAUSE)
    span = slots // KEY_PIECES
    k_copies = [
        pltpu.make_async_copy(
            k_hbm.at[pl.ds(i * span, span)], k_vmem.at[pl.ds(i * span, span)], k_sem.at[i]
        )
        for i in range(KEY_PIECES)
    ]
    v_copies = []

    def source(item):
        return item if item < KEY_PIECES else source(item - WINDOW)

    for j in range(pairs):
        cuts = VALUE_PIECES[min(j, 1)]
        unit, at = slots // sum(cuts), 0
        for size in cuts:
            pages = pl.ds(at, size * unit)
            v_copies.append(
                (
                    j,
                    at,
                    size * unit,
                    pltpu.make_async_copy(
                        v_hbm.at[pages, pl.ds(2 * j, 2)],
                        v_vmem.at[pages, pl.ds(2 * j, 2)],
                        k_sem.at[source(KEY_PIECES + len(v_copies))],
                    ),
                )
            )
            at += size * unit
    unstarted = k_copies + [copy for _, _, _, copy in v_copies]

    def begin(count):
        for _ in range(min(count, len(unstarted))):
            unstarted.pop(0).start()

    begin(WINDOW)

    def stat_copy(i):
        return pltpu.make_async_remote_copy(
            src_ref=stat_out.at[i],
            dst_ref=stat_in.at[me],
            send_sem=stat_send,
            recv_sem=stat_recv,
            device_id={"seq": targets[i], "head": gate},
            device_id_type=MESH,
        )

    def num_copy(j, i):
        return pltpu.make_async_remote_copy(
            src_ref=num_out.at[j, i],
            dst_ref=num_in.at[j, me],
            send_sem=num_send,
            recv_sem=num_recv.at[j, late],
            device_id={"seq": targets[i], "head": gate},
            device_id_type=MESH,
        )

    def near_copy(src, dst, send, recv):
        return pltpu.make_async_remote_copy(
            src_ref=src,
            dst_ref=dst,
            send_sem=send,
            recv_sem=recv,
            device_id={"seq": near, "head": 0},
            device_id_type=MESH,
        )

    def fin_copy(h, seq):
        return pltpu.make_async_remote_copy(
            src_ref=done_ref,
            dst_ref=out_ref.at[pl.ds(rank * share, share)],
            send_sem=fin_send,
            recv_sem=fin_recv,
            device_id={"seq": seq, "head": h},
            device_id_type=MESH,
        )

    def bytes_of(ref, sem):
        return pltpu.make_async_remote_copy(
            src_ref=ref,
            dst_ref=ref,
            send_sem=sem,
            recv_sem=sem,
            device_id={"seq": targets[0], "head": gate},
            device_id_type=MESH,
        )

    def iota(shape, dim):
        return lax.broadcasted_iota(jnp.int32, shape, dim)

    small[0].wait()
    small[1].wait()
    entry = iota((1, pool), 1)
    live = jnp.zeros((1, pool), jnp.int32)
    owner_seq = jnp.zeros((1, pool), jnp.int32)
    for b in range(batch):
        past = entry >= b * table_width
        left = jnp.clip(len_smem[b] - page * (entry - b * table_width), 0, page)
        live = jnp.where(past, left, live)
        owner_seq = jnp.where(past, b, owner_seq)
    hit = pt_vmem[...].reshape(1, pool) == me * slots + iota((slots, pool), 0)
    seq_col = jnp.sum(jnp.where(hit, owner_seq.astype(f32), 0.0), axis=1, keepdims=True)
    live_col = jnp.sum(jnp.where(hit, live.astype(f32), 0.0), axis=1, keepdims=True)
    seq_wide = jnp.broadcast_to(seq_col, (slots, page))
    slot_seq[...] = seq_wide
    slot_live[...] = jnp.broadcast_to(live_col, (slots, page))
    lane = iota((rows, page), 1)
    lane_f = lane.astype(f32)
    diagonal = iota((slots, page), 0) == iota((slots, page), 1)
    seq_row = jnp.sum(jnp.where(diagonal, seq_wide, 0.0), axis=0, keepdims=True)
    seq_row = jnp.where(iota((1, page), 1) < slots, seq_row, -1.0)
    row_vmem[...] = jnp.clip(seq_row.astype(jnp.int32), 0, batch - 1)
    row_copy = pltpu.make_async_copy(row_vmem, row_smem, small_sem.at[0])
    row_copy.start()
    seq_row = jnp.broadcast_to(seq_row, (rows, page))

    small[2].wait()
    column = iota((heads, 2 * batch * heads), 1)
    line = iota((heads, 2 * batch * heads), 0)
    match = column // (batch * heads) == line % rows // half
    mark = jnp.where((column % heads == line) & match, column % (batch * heads) // heads, -1)
    mark = mark.astype(f32)
    queries = q_raw[...].reshape(batch * heads, head_dim)
    blank = jnp.zeros_like(queries)
    queries = jnp.concatenate(
        [
            jnp.concatenate([queries, blank], axis=1),
            jnp.concatenate([blank, queries], axis=1),
        ],
        axis=0,
    )
    for unit in range(2):
        pltpu.matmul_push_rhs(queries, staging_register=0, mxu_index=unit)
    group = slots // len(pick_acc)
    for i, acc in enumerate(pick_acc):
        pick = []
        for pp in range(i * group // 2, (i + 1) * group // 2):
            for j in range(pairs):
                for p in (2 * pp, 2 * pp + 1):
                    seq = slot_seq[p : p + 1, :]
                    seq = jnp.concatenate([seq, seq], axis=1)
                    pick.append(jnp.where(mark[j * rows : (j + 1) * rows] == seq, 1.0, 0.0))
        pick = jnp.concatenate(pick, axis=0).astype(bf16)
        pltpu.matmul_acc_lhs(acc, pick, load_staged_rhs=0 if i < 2 else None)
    def store_picks(i):
        found = pltpu.matmul_pop(pick_acc[i]).astype(bf16)
        here = pl.ds(i * group * heads, group * heads)
        picked[0, here] = found[:, :head_dim]
        picked[1, here] = found[:, head_dim:]

    store_picks(0)
    wide = (iota((batch * rows, page), 0) // rows).astype(f32)
    each = iota((batch, page), 0).astype(f32)
    peaks = {(j, b): jnp.full((rows, page), VERY_LOW, f32) for j in range(pairs) for b in range(batch)}
    sums = [jnp.zeros((rows, page), f32) for _ in range(pairs)]

    def prepare(p):
        choose[p] = jnp.where(wide == slot_seq[p : p + 1, :], 1.0, 0.0).astype(bf16)
        bias[p] = jnp.where(each == slot_seq[p : p + 1, :], 0.0, VERY_LOW)

    def score(pp, j):
        both = [
            k_vmem[2 * pp : 2 * pp + 2, 2 * j + g].reshape(2 * page, head_dim) for g in range(2)
        ]
        tile = pp * pairs + j
        register = tile // 2 % 2
        pltpu.matmul_push_rhs(
            jnp.concatenate(both, axis=1),
            staging_register=register,
            mxu_index=tile % 2,
            transpose=True,
        )
        pltpu.matmul_acc_lhs(
            score_acc[tile],
            jnp.concatenate([picked[g, pl.ds(tile * 2 * rows, 2 * rows)] for g in range(2)], axis=1),
            load_staged_rhs=register,
        )

    def scores(pp, j):
        found = pltpu.matmul_pop(score_acc[pp * pairs + j])
        return [found[i * rows : (i + 1) * rows, i * page : (i + 1) * page] for i in range(2)]

    def settle(p, j, s):
        s = jnp.where(lane_f < slot_live[p : p + 1, :], s * factor, VERY_LOW)
        soft[p, j] = s
        for b in range(batch):
            peaks[j, b] = jnp.maximum(peaks[j, b], s + bias[p, b : b + 1, :])

    for i in range(KEY_PIECES + 1):
        if i < KEY_PIECES:
            k_copies[i].wait()
            begin(1)
            for pp in range(i * span // 2, (i + 1) * span // 2):
                for j in range(pairs):
                    score(pp, j)
            if i + 1 < KEY_PIECES:
                store_picks(i + 1)
            for p in range(i * span, (i + 1) * span):
                prepare(p)
        if i > 0:
            for pp in range((i - 1) * span // 2, i * span // 2):
                for j in range(pairs):
                    for k, found in enumerate(scores(pp, j)):
                        settle(2 * pp + k, j, found)

    row_copy.wait()
    for key in peaks:
        j, b = key
        peaks[key] = jnp.maximum(jnp.max(peaks[key], axis=1, keepdims=True), FLOOR)
        crest[b, j] = jnp.broadcast_to(peaks[key], (rows, page))

    def soften(j, p):
        seq = jnp.clip(row_smem[0, p], 0, batch - 1)
        w = jnp.exp2(soft[p, j] - crest[seq, j])
        sums[j] = jnp.where(lane == p, jnp.sum(w, axis=1, keepdims=True), sums[j])
        w = jnp.concatenate([w] * 2, axis=0).astype(bf16)
        w = jnp.concatenate([w] * (batch // 2), axis=0)
        spread[j, p] = w * choose[p]

    stats = [jnp.zeros((rows, page), f32) for _ in range(parts)]
    inverse = {}

    def account(j):
        for b in range(batch):
            total = jnp.where(seq_row == float(b), sums[j], 0.0)
            total = jnp.sum(total, axis=1, keepdims=True)
            some = total > 0.0
            safe = jnp.where(some, total, 1.0)
            level = jnp.where(some, peaks[j, b] + jnp.log2(safe), VERY_LOW)
            inverse[j, b] = jnp.broadcast_to(1.0 / safe, (rows, head_dim))
            i, local = b // share, b % share
            stats[i] = jnp.where(lane == j * share + local, level, stats[i])

    upper = iota((batch * rows, head_dim), 0) % rows < half

    def gather(j, at, size):
        for pp in range(at // 2, (at + size) // 2):
            both = [
                v_vmem[2 * pp : 2 * pp + 2, 2 * j + g].reshape(2 * page, head_dim)
                for g in range(2)
            ]
            register = pp // 2 % 2
            pltpu.matmul_push_rhs(
                jnp.concatenate(both, axis=1), staging_register=register, mxu_index=pp % 2
            )
            pltpu.matmul_acc_lhs(
                value_acc[2 * j + pp % 2],
                jnp.concatenate([spread[j, 2 * pp], spread[j, 2 * pp + 1]], axis=1),
                load_staged_rhs=register,
            )

    def merge(j):
        found = pltpu.matmul_pop(value_acc[2 * j]) + pltpu.matmul_pop(value_acc[2 * j + 1])
        return jnp.where(upper, found[:, :head_dim], found[:, head_dim:])

    def post(start, keep):
        @pl.when(jnp.logical_not(mine))
        def _():
            for i in range(parts):
                start(i)

        @pl.when(mine)
        def _():
            for i, o in enumerate(owners[gate]):
                @pl.when(me != o)
                def _():
                    start(i)

                @pl.when(me == o)
                def _():
                    keep(i)

    def post_stats():
        for i in range(parts):
            stat_out[i] = stats[i]
        pl.semaphore_wait(barrier, jnp.where(mine, parts - 1, parts) + late)

        def keep(i):
            stat_in[me] = stat_out[i]

        post(lambda i: stat_copy(i).start(), keep)

    def post_numer(j, numer):
        scale = jnp.concatenate([inverse[j, b] for b in range(batch)], axis=0)
        num_out[j] = (numer * scale).reshape(parts, share * rows, head_dim)

        def keep(i):
            num_in[j, me] = num_out[j, i]

        @pl.when(is_far)
        def _():
            near_copy(num_out.at[j], far_in.at[j], far_send, far_recv).start()

        post(lambda i: num_copy(j, i).start(), keep)

    first = v_copies[0][2]
    for p in range(first):
        soften(0, p)
    owed = None
    for j, at, size, copy in v_copies:
        copy.wait()
        begin(1)
        gather(j, at, size)
        if j == 0:
            for p in range(at + size, min(at + size + first, slots)):
                soften(0, p)
            for other in range(1, pairs):
                for p in range(at, at + size):
                    soften(other, p)
            if at + size == slots:
                for other in range(pairs):
                    account(other)
        if owed is not None:
            if owed == 0:
                post_stats()
            post_numer(owed, merge(owed))
        owed = j if at + size == slots else None
    post_numer(owed, merge(owed))

    def combine(h):
        senders = n - 1 if h == gate else n
        bytes_of(stat_in.at[pl.ds(0, senders)], stat_recv).wait_recv()
        levels = stat_in[...]
        scales = jnp.exp2(levels - jnp.max(levels, axis=0, keepdims=True))
        scales = scales / jnp.sum(scales, axis=0, keepdims=True)
        columns = {}
        for s in range(n):
            for at in range(pairs * share):
                columns[s, at] = jnp.broadcast_to(scales[s][:, at : at + 1], (rows, head_dim))
        if h != gate:
            rest_scale[...] = scales[far]
            near_copy(rest_scale, scale_in.at[rank], scale_send, scale_recv).start()

        def term(s, j, local):
            here = pl.ds(local * rows, rows)
            return columns[s, j * share + local] * num_in[j, s, here, :]

        blocks = {}
        for j in range(pairs):
            bytes_of(num_in.at[j, pl.ds(0, n - 1)], num_recv.at[j, 0]).wait_recv()
            for local in range(share):
                blocks[j, local] = sum(
                    term(s, j, local) for s in range(n) if h == gate or s != far
                )
            if h != gate:
                for local in range(share):
                    rest[j, pl.ds(local * rows, rows), :] = blocks[j, local]
                near_copy(rest.at[j], rest_in.at[j, rank], rest_send, rest_recv).start()
        if h != gate:
            for j in range(pairs):
                bytes_of(num_in.at[j, pl.ds(0, 1)], num_recv.at[j, 1]).wait_recv()
                for local in range(share):
                    blocks[j, local] = blocks[j, local] + term(far, j, local)
        for local in range(share):
            whole = [blocks[j, local] for j in range(pairs)]
            whole = jnp.concatenate(whole, axis=0).astype(out_ref.dtype)
            done_ref[local] = whole
            if h == gate:
                out_ref[rank * share + local] = whole
        for seq in members(h) if h == gate else range(1, n):
            fin_copy(h, seq).start()

    for h in range(sides):
        @pl.when(serves[h])
        def _():
            combine(h)

    @pl.when(jnp.logical_not(mine))
    def _():
        bytes_of(stat_out, stat_send).wait_send()
        bytes_of(num_out, num_send).wait_send()

    @pl.when(is_far)
    def _():
        bytes_of(num_out, far_send).wait_send()

    @pl.when(jnp.logical_not(mine | is_near))
    def _():
        bytes_of(out_ref, fin_recv).wait_recv()

    @pl.when(is_near)
    def _():
        bytes_of(scale_in, scale_recv).wait_recv()
        columns = {}
        for i in range(parts):
            for at in range(pairs * share):
                columns[i, at] = jnp.broadcast_to(
                    scale_in[i][:, at : at + 1], (rows, head_dim)
                )
        bytes_of(rest_in, rest_recv).wait_recv()
        bytes_of(far_in, far_recv).wait_recv()
        for i in range(parts):
            for local in range(share):
                here = pl.ds(local * rows, rows)
                whole = [
                    rest_in[j, i, here, :] + columns[i, j * share + local] * far_in[j, i, here, :]
                    for j in range(pairs)
                ]
                whole = jnp.concatenate(whole, axis=0).astype(out_ref.dtype)
                out_ref[i * share + local] = whole

    @pl.when(mine)
    def _():
        if parts > 1:
            bytes_of(stat_out.at[pl.ds(0, parts - 1)], stat_send).wait_send()
            bytes_of(num_out.at[:, pl.ds(0, parts - 1)], num_send).wait_send()
            bytes_of(out_ref.at[pl.ds(0, (parts - 1) * share)], fin_recv).wait_recv()

    for h in range(sides):
        @pl.when(serves[h])
        def _():
            bytes_of(tally, fin_send).wait_send()
            if h != gate:
                bytes_of(rest_scale, scale_send).wait_send()
                bytes_of(rest, rest_send).wait_send()


def scoped(n, sides, table_width, owners, batch, heads, slots, pairs, *refs):
    rows = heads // pairs
    pieces = KEY_PIECES
    accs = []
    for i in range(pieces):
        accs.append(pltpu.ACC(i % 2)((slots * heads // pieces, 256), jnp.float32))
    tiles = slots // 2 * pairs
    for i in range(tiles):
        accs.append(pltpu.ACC(i % 2)((2 * rows, 256), jnp.float32))
    for i in range(2 * pairs):
        accs.append(pltpu.ACC(i % 2)((batch * rows, 256), jnp.float32))

    def body(*accs):
        attend(
            n,
            sides,
            table_width,
            owners,
            accs[:pieces],
            accs[pieces : pieces + tiles],
            accs[pieces + tiles :],
            *refs,
        )

    pl.run_scoped(body, *accs)


def shards(n, sides, owners, query_rows, cache_keys, cache_values, page_table, seq_lengths):
    slots, kv_heads, page, head_dim = cache_keys.shape
    batch, heads, _ = query_rows.shape
    pool = page_table.shape[0]
    rows, pairs = 2 * heads // kv_heads, kv_heads // 2
    parts = len(owners[0])
    share = batch // parts
    f32, bf16 = jnp.float32, jnp.bfloat16
    hbm = pl.BlockSpec(memory_space=pl.ANY)
    dma = pltpu.SemaphoreType.DMA
    return pl.pallas_call(
        functools.partial(scoped, n, sides, pool // batch, owners, batch, heads, slots, pairs),
        out_shape=pltpu.VMEM((batch, heads, head_dim), bf16),
        in_specs=[hbm] * 5,
        out_specs=pl.BlockSpec(memory_space=pltpu.VMEM),
        scratch_shapes=[
            pltpu.VMEM((batch, heads, head_dim), bf16),
            pltpu.VMEM((pool,), jnp.int32),
            pltpu.SMEM((batch,), jnp.int32),
            pltpu.VMEM((slots, kv_heads, page, head_dim), bf16),
            pltpu.VMEM((slots, kv_heads, page, head_dim), bf16),
            pltpu.VMEM((slots, page), f32),
            pltpu.VMEM((slots, page), f32),
            pltpu.VMEM((2, slots * heads, head_dim), bf16),
            pltpu.VMEM((slots, batch * rows, page), bf16),
            pltpu.VMEM((slots, pairs, rows, page), f32),
            pltpu.VMEM((pairs, slots, batch * rows, page), bf16),
            pltpu.VMEM((slots, batch, page), f32),
            pltpu.VMEM((batch, pairs, rows, page), f32),
            pltpu.VMEM((1, page), jnp.int32),
            pltpu.SMEM((1, page), jnp.int32),
            pltpu.VMEM((share, heads, head_dim), bf16),
            pltpu.VMEM((n - 1, share, heads, head_dim), bf16),
            pltpu.VMEM((rows, page), f32),
            pltpu.VMEM((pairs, share * rows, head_dim), f32),
            pltpu.VMEM((parts, rows, page), f32),
            pltpu.VMEM((pairs, parts, share * rows, head_dim), f32),
            pltpu.VMEM((pairs, parts, share * rows, head_dim), f32),
            pltpu.VMEM((parts, rows, page), f32),
            pltpu.VMEM((n, rows, page), f32),
            pltpu.VMEM((pairs, parts, share * rows, head_dim), f32),
            pltpu.VMEM((pairs, n, share * rows, head_dim), f32),
            dma((3,)),
            dma((KEY_PIECES,)),
            dma,
            dma,
            dma,
            dma((pairs, 2)),
            dma,
            dma,
            dma,
            dma,
            dma,
            dma,
            dma,
            dma,
        ],
        compiler_params=pltpu.CompilerParams(collective_id=0, has_side_effects=True),
    )(query_rows, cache_keys, cache_values, page_table, seq_lengths)


def owners_of(n, sides):
    even = tuple(range(0, n, n // 4))
    return tuple(tuple(o + h for o in even) for h in range(sides))


def solution(mesh):
    n = mesh.shape["seq"]
    owners = owners_of(n, mesh.shape["head"])
    in_specs = (
        P("grp", "head", None),
        P(("grp", "seq"), "head", None, None),
        P(("grp", "seq"), "head", None, None),
        P("grp"),
        P("grp"),
    )
    return jax.shard_map(
        functools.partial(shards, n, mesh.shape["head"], owners),
        mesh=mesh,
        in_specs=in_specs,
        out_specs=P("grp", "head", None),
        check_vma=False,
    )
```
